256 devices in a mesh: agent: 32 (over x, y, core), res: 8 (over z).
Axes of the slice: x: 4, y: 4, z: 8, core: 2. Of those that a mesh axis runs over, the one named last changes fastest.
Arguments:
- linear_cost: float32 [8192, 2048], P('agent', 'res'), may hold values from -6 to 6
- agent_type: int32 [8192], P('agent'), may hold values from 0 to 3, as said below
- block_mask: int32 [8192, 16], P('agent', 'res'), may hold values 0 or 1
- inverses: bfloat16 [4, 2048, 2048], P(None, 'res'), as said below
- cost_weight: float32 [2048], P('res'), may hold values from 0.5 to 8
- target: float32 [2048], P('res'), may hold values from -6 to 6
Outputs:
- usage: float32 [8192, 2048], P('agent', 'res')
- shared: float32 [2048], P('res')
- prices: float32 [2048], P('res')
- primal_norm: float32 [5], replicated
- dual_norm: float32 [5], replicated
The draws below stay inside these ranges and needn't reach their ends.
Inputs may be any that keep to these rules, and one draw needn't show every extreme that they name: Each inverses[k] is exactly symmetric: inverses[k, i, j] equals inverses[k, j, i]. `agent_type`: each aligned block of 256 agents (the agents held by one device along the agent axis) holds exactly 64 agents of each type, in no particular order.
All inputs are finite; a program needn't handle non-finite values. No bound on the sum of `block_mask` on one device may be relied on, other than what follows from the above.
Results may differ from the reference program's by a relative error of at most 0.0039.
Values may be sent and summed in bfloat16 or wider, within the bound.
A program may use at most 64 MiB of HBM per device.

```python
import math
import jax
import jax.numpy as jnp
from jax import lax

R = 2048
BLK = 128
TYPES = 4
ITERS = 5
AG_DEV = 256
AGENTS = 8192
NBLK = 16


def draw_agent_type(key, part):
    block_count = AGENTS // AG_DEV
    keys = jax.random.split(jax.random.fold_in(key, 29), block_count)
    base = (jnp.arange(AG_DEV, dtype=jnp.int32) % TYPES).astype(jnp.int32)
    blocks = jax.vmap(lambda single: jax.random.permutation(single, base))(keys)
    return blocks.reshape(AGENTS).astype(jnp.int32)


def draw_inverses(key, part):
    first_key, second_key = jax.random.split(jax.random.fold_in(key, 17), 2)
    gauss = jax.random.normal(first_key, (TYPES, R, R), jnp.float32)
    off_scale = 0.15
    diagonal = jax.random.uniform(second_key, (TYPES, R), jnp.float32, 0.4, 1.0)
    symmetric = (gauss + jnp.swapaxes(gauss, 1, 2)) * (off_scale / jnp.sqrt(2.0 * R))
    identity = jnp.eye(R, dtype=jnp.float32)
    matrix = symmetric * (1.0 - identity) + diagonal[:, :, None] * identity
    return matrix.astype(jnp.bfloat16)


def with_ends(values, rng, low, high):
    longest = values.shape.index(max(values.shape))
    spots = []
    for shift in (0, 1):
        where = [jax.random.randint(jax.random.fold_in(rng, axis), (), 0, length) for axis, length in enumerate(values.shape)]
        where[longest] = (where[longest] + shift) % values.shape[longest]
        spots.append(tuple(where))
    return values.at[spots[0]].set(low).at[spots[1]].set(high)


def level_of(stream_key, extent, cuts, smallest, largest):
    gain, own = 1.0, jax.random.fold_in(stream_key, 6)
    for dim, parts in cuts:
        heights = jnp.exp(jax.random.uniform(jax.random.fold_in(own, dim), (parts,), jnp.float32, smallest / len(cuts), largest / len(cuts)))
        gain = gain * jnp.repeat(heights, extent[dim] // parts).reshape([-1 if axis == dim else 1 for axis in range(len(extent))])
    return gain


def scatter_about(own_key, shape, spread, reach, shards=(), kind=jnp.bfloat16):
    drawn = spread * jax.random.normal(own_key, shape, jnp.float32)
    if shards:
        drawn = drawn * level_of(own_key, shape, shards, -0.22, 0.18)
    return jnp.clip(drawn, -reach, reach).astype(kind)


def setup_inputs(seed: int = 0) -> dict:
    streams_of = jax.random.split(jax.random.key(seed), 7)
    return {
        "linear_cost": scatter_about(streams_of[0], (AGENTS, R), 1.0, 6.0, ((0, 32), (1, 8)), jnp.float32),
        "agent_type": draw_agent_type(jax.random.fold_in(streams_of[6], 71), 0),
        "block_mask": with_ends((jax.random.randint(streams_of[2], (AGENTS, NBLK), 0, 4) < 3).astype(jnp.int32), jax.random.fold_in(streams_of[2], 1), 0, 1),
        "inverses": draw_inverses(jax.random.fold_in(streams_of[6], 71), 0),
        "cost_weight": jnp.clip(jnp.exp(math.log(8.0) - 2.7725887 * jax.random.uniform(streams_of[4], (R,), jnp.float32) ** level_of(streams_of[4], (R,), ((0, 8),), -0.2, 0.2)), 0.5, 8.0),
        "target": scatter_about(streams_of[5], (R,), 1.0, 6.0, ((0, 8),), jnp.float32),
    }


penalty = 1.0
eps = 1e-06

def reference(linear_cost, agent_type, block_mask, inverses, cost_weight, target):
    count = linear_cost.shape[0]
    group_rows = count // TYPES
    order = jnp.argsort(agent_type, stable=True).astype(jnp.int32)
    restore = jnp.argsort(order, stable=True).astype(jnp.int32)
    matrices = inverses.astype(jnp.float32)
    expand = jnp.repeat(block_mask.astype(jnp.float32), BLK, axis=1)
    usage = jnp.zeros(linear_cost.shape, jnp.float32)
    mean_usage = jnp.zeros((R,), jnp.float32)
    shared = jnp.zeros((R,), jnp.float32)
    prices = jnp.zeros((R,), jnp.float32)
    primal_list = []
    dual_list = []
    for iteration in range(ITERS):
        rhs = (penalty * (usage - mean_usage + shared - prices) - linear_cost).astype(jnp.bfloat16)
        grouped = rhs[order].astype(jnp.float32).reshape(TYPES, group_rows, R)
        product = jnp.einsum('tar,trw->taw', grouped, matrices).reshape(count, R)
        new_usage = product[restore] * expand
        dual2 = penalty * penalty * jnp.sum((new_usage - usage) ** 2)
        usage = new_usage
        mean_usage = lax.optimization_barrier(jnp.sum(usage, axis=0)) / count
        shared = (cost_weight * target + penalty * (prices + mean_usage)) / (cost_weight + penalty)
        prices = prices + mean_usage - shared
        primal2 = count * jnp.sum((mean_usage - shared) ** 2)
        primal_list.append(jnp.sqrt(primal2 + eps))
        dual_list.append(jnp.sqrt(dual2 + eps))
    return (usage, shared, prices, jnp.stack(primal_list), jnp.stack(dual_list))
```

```python
import functools

import jax
import jax.numpy as jnp
from jax import lax
from jax.experimental import pallas as pl
from jax.experimental.pallas import tpu as pltpu
from jax.sharding import PartitionSpec as P

ITERS = 5
AGENTS = 8192
EPS = 1e-06
MESH = pl.DeviceIdType.MESH
F32 = jnp.float32
BF16 = jnp.bfloat16


def three_parts(value):
    high = value.astype(BF16).astype(F32)
    rest = value - high
    mid = rest.astype(BF16).astype(F32)
    return high, mid, rest - mid


def kernel(
    cost_ref, type_ref, mask_ref, weight_ref, target_ref, inv_ref,
    usage_out, shared_out, prices_out, primal_out, dual_out,
    mats, order, packed, rows, expand, usage, rhs, vectors, plane, lines, back,
    mat_load, z_send, z_recv, one_send, one_recv, two_send, two_recv, core_send, core_recv,
    row_send, row_recv, plane_send, plane_recv, line_send, line_recv, back_send, back_recv,
):
    agent, z = lax.axis_index("agent"), lax.axis_index("res")
    x, y, c = agent // 8, (agent // 2) % 4, agent % 2
    kind = z % 4
    first, second = x * (1 - c) + y * c, y * (1 - c) + x * c
    place = x * 4 + y

    def at(px, py, pc, pz):
        return (px * 8 + py * 2 + pc, pz)

    def along(step_one, step_two):
        one, two = (first + step_one) % 4, (second + step_two) % 4
        return at(one * (1 - c) + two * c, two * (1 - c) + one * c, c, z)

    def copy(src, dst, send, recv, device):
        return pltpu.make_async_remote_copy(src, dst, send, recv, device_id=device, device_id_type=MESH)

    def plane_peer(e):
        other = (place + e) % 16
        return at(other // 4, other % 4, c, z)

    def line_peer(e):
        other = (c * 8 + z + e) % 16
        return other // 8, other % 8

    barrier = pltpu.get_barrier_semaphore()

    def greet(e, carry):
        pl.semaphore_signal(barrier, inc=1, device_id=plane_peer(e), device_id_type=MESH)
        pc, pz = line_peer(e)
        pl.semaphore_signal(barrier, inc=1, device_id=at(x, y, pc, pz), device_id_type=MESH)
        return carry

    lax.fori_loop(1, 16, greet, 0)
    own_loads = [
        pltpu.make_async_copy(
            inv_ref.at[kind, pl.ds(q * 16, 16), pl.ds(h * 1024, 1024)],
            mats.at[h, z, q // 4, q % 4],
            mat_load.at[h * 16 + q],
        )
        for h in range(2)
        for q in range(16)
    ]
    for load in own_loads:
        load.start()
    pl.semaphore_wait(barrier, 30)

    def z_copy(d):
        far = (z + d) % 8
        return copy(
            inv_ref.at[far % 4, pl.ds((first * 4 + second) * 16, 16), pl.ds(pl.multiple_of(c * 1024, 1024), 1024)],
            mats.at[c, z, first, second],
            z_send.at[d],
            z_recv.at[d],
            at(x, y, c, far),
        )

    for d in (4, 3, 5, 2, 6, 1, 7):
        z_copy(d).start()

    kinds = type_ref[...]
    is_kind = (lax.broadcasted_iota(jnp.int32, (16, 256), 0) == kinds).astype(F32)
    before = (
        lax.broadcasted_iota(jnp.int32, (256, 256), 0) < lax.broadcasted_iota(jnp.int32, (256, 256), 1)
    ).astype(BF16)
    ahead = jnp.dot(is_kind.astype(BF16), before, preferred_element_type=F32)
    spot = kinds * 64 + jnp.sum(is_kind * ahead, axis=0, keepdims=True).astype(jnp.int32)
    order[...] = (lax.broadcasted_iota(jnp.int32, (256, 256), 0) == spot).astype(F32).astype(BF16)
    cost = jnp.dot(order[...], cost_ref[...].astype(BF16), preferred_element_type=F32).astype(BF16)
    extra = jnp.concatenate(
        [mask_ref[...].astype(F32), jnp.zeros((14, 256), F32)], axis=0
    ).astype(BF16)
    masks = lax.dot_general(extra, order[...], (((1,), (1,)), ((), ())), preferred_element_type=F32)
    line = lax.broadcasted_iota(jnp.int32, (16, 256), 0)
    lane = lax.broadcasted_iota(jnp.int32, (16, 256), 1)
    tail = jnp.zeros((16, 256), F32)
    for r, part in enumerate(three_parts(weight_ref[...]) + three_parts(target_ref[...])):
        tail = jnp.where(line == 2 + r, part, tail)
    for t in range(4):
        packed[t, :64] = cost[t * 64 : (t + 1) * 64]
        turned = masks if t == 0 else pltpu.roll(masks, 256 - 64 * t, 1)
        packed[t, 64:] = jnp.where((line < 2) & (lane < 64), turned, tail).astype(BF16)

    def row_copy(e):
        pc, pz = line_peer(e)
        return copy(
            packed.at[pz % 4], rows.at[z, c], row_send.at[e], row_recv.at[e], at(x, y, pc, pz)
        )

    def start_rows(e, carry):
        row_copy(e).start()
        return carry

    lax.fori_loop(1, 16, start_rows, 0)
    rows[z, c] = packed[kind]

    def part(d):
        return mats.at[c, (z - d + 8) % 8]

    def one_copy(d, s):
        block = part(d).at[first, second]
        return copy(block, block, one_send.at[d, s], one_recv.at[d, s], along(s, 0))

    def two_copy(d, s):
        block = part(d).at[:, second]
        return copy(block, block, two_send.at[d, s], two_recv.at[d, s], along(0, s))

    def core_copy(d):
        return copy(part(d), part(d), core_send.at[d], core_recv.at[d], at(x, y, 1 - c, z))

    for d in (1, 7, 2, 6, 3, 5, 4):
        z_copy(d).wait_recv()
        for s in (2, 1, 3):
            one_copy(d, s).start()
    for d in (1, 7, 2, 6, 3, 5, 4):
        for s in (2, 1, 3):
            one_copy(d, s).wait_recv()
        for s in (2, 1, 3):
            two_copy(d, s).start()

    def wait_rows(e, carry):
        row_copy(e).wait_recv()
        return carry

    lax.fori_loop(1, 16, wait_rows, 0)
    wide = (lax.broadcasted_iota(jnp.int32, (16, 256), 1) // 128 == line).astype(F32).astype(BF16)
    for j in range(8):
        ends = rows[j, 0, 64:].astype(F32)
        vectors[0, j : j + 1] = ends[2:3] + ends[3:4] + ends[4:5]
        vectors[1, j : j + 1] = ends[5:6] + ends[6:7] + ends[7:8]
        for half in range(2):
            here = rows[j, half, 64:, :128]
            spread = lax.dot_general(here, wide, (((0,), (0,)), ((), ())), preferred_element_type=F32)
            expand[j, half * 64 : half * 64 + 64] = spread[:64]

    usage[...] = jnp.zeros_like(usage)
    for v in (2, 3, 4):
        vectors[v] = jnp.zeros((8, 256), F32)

    for d in (1, 7, 2, 6, 3, 5, 4):
        for s in (2, 1, 3):
            two_copy(d, s).wait_recv()
        core_copy(d).start()
    for load in own_loads:
        load.wait()
    for d in (1, 7, 2, 6, 3, 5, 4):
        core_copy(d).wait_recv()

    norm_lane = lax.broadcasted_iota(jnp.int32, (1, 128), 1)

    def back_copy(e):
        far = (z + e) % 8
        return copy(
            usage.at[far, pl.ds(pl.multiple_of(c * 64, 64), 64)],
            back.at[kind],
            back_send.at[e],
            back_recv.at[e],
            at(x, y, c, far),
        )

    def iteration(it, norms):
        primal_norms, dual_norms = norms
        par = it

        def right_side(j, carry):
            shift = vectors[3, pl.ds(j, 1)] - vectors[2, pl.ds(j, 1)] - vectors[4, pl.ds(j, 1)]
            costs = rows[j, :, :64].astype(F32).reshape(128, 256)
            rhs[:, pl.ds(pl.multiple_of(j * 256, 256), 256)] = (usage[j] + shift - costs).astype(BF16)
            return carry

        lax.fori_loop(0, 8, right_side, 0)

        def product(j, change):
            block = mats[j // 4, :, :, :, :, pl.ds(pl.multiple_of((j % 4) * 256, 256), 256)].reshape(2048, 256)
            fresh = jnp.dot(rhs[...], block, preferred_element_type=F32) * expand[j]
            gap = fresh - usage[j]
            usage[j] = fresh
            plane[par, place, pl.ds(j, 1)] = jnp.sum(fresh, axis=0, keepdims=True)
            return change + jnp.sum(gap * gap, axis=0, keepdims=True)

        change = lax.fori_loop(0, 8, product, jnp.zeros((1, 256), F32))
        plane[par, place, 8:] = jnp.broadcast_to(change, (8, 256))

        def plane_copy(e):
            return copy(
                plane.at[par, place], plane.at[par, place], plane_send.at[e], plane_recv.at[par, e], plane_peer(e)
            )

        def start_plane(e, carry):
            plane_copy(e).start()
            return carry

        def end_plane(e, carry):
            plane_copy(e).wait()
            return carry

        lax.fori_loop(1, 16, start_plane, 0)
        lax.fori_loop(1, 16, end_plane, 0)
        lines[par, kind] = jnp.sum(plane[par], axis=0)

        def line_copy(e):
            return copy(
                lines.at[par, kind], lines.at[par, kind], line_send.at[e], line_recv.at[par, e],
                at(x, y, c, (z + (1, 7, 2)[e]) % 8),
            )

        for e in range(3):
            line_copy(e).start()
        for e in range(3):
            line_copy(e).wait()
        total = jnp.sum(lines[par], axis=0)
        mean = total[:8] * (1.0 / AGENTS)
        prices = vectors[4]
        shared = (vectors[0] * vectors[1] + (prices + mean)) / (vectors[0] + 1.0)
        vectors[2] = mean
        vectors[3] = shared
        vectors[4] = prices + mean - shared
        gap = mean - shared
        primal = float(AGENTS) * jnp.sum(gap * gap)
        dual = jnp.sum(total[8:9])
        return (
            jnp.where(norm_lane == it, primal, primal_norms),
            jnp.where(norm_lane == it, dual, dual_norms),
        )

    zero = jnp.zeros((1, 128), F32)
    primal_norms, dual_norms = lax.fori_loop(0, ITERS, iteration, (zero, zero))
    for e in (1, 7, 2):
        back_copy(e).start()
    back[kind] = usage[z, pl.ds(pl.multiple_of(c * 64, 64), 64)]
    primal_out[...] = jnp.sqrt(primal_norms + EPS)
    dual_out[...] = jnp.sqrt(dual_norms + EPS)
    shared_out[...] = vectors[3, pl.ds(z, 1)]
    prices_out[...] = vectors[4, pl.ds(z, 1)]
    for e in (1, 7, 2):
        back_copy(e).wait_recv()
    result = jnp.zeros((256, 256), F32)
    for piece in three_parts(back[...].reshape(256, 256)):
        result += lax.dot_general(
            order[...], piece.astype(BF16), (((0,), (0,)), ((), ())), preferred_element_type=F32
        )
    usage_out[...] = result

    def end_rows(e, carry):
        row_copy(e).wait_send()
        return carry

    lax.fori_loop(1, 16, end_rows, 0)
    for d in range(1, 8):
        z_copy(d).wait_send()
        for s in (1, 2, 3):
            one_copy(d, s).wait_send()
            two_copy(d, s).wait_send()
        core_copy(d).wait_send()
    for e in (1, 7, 2):
        back_copy(e).wait_send()


def on_device(linear_cost, agent_type, block_mask, inverses, cost_weight, target):
    vmem = pl.BlockSpec(memory_space=pltpu.VMEM)
    dma = pltpu.SemaphoreType.DMA
    usage, shared, prices, primal, dual = pl.pallas_call(
        kernel,
        out_shape=(
            jax.ShapeDtypeStruct((256, 256), F32),
            jax.ShapeDtypeStruct((1, 256), F32),
            jax.ShapeDtypeStruct((1, 256), F32),
            jax.ShapeDtypeStruct((1, 128), F32),
            jax.ShapeDtypeStruct((1, 128), F32),
        ),
        in_specs=[vmem] * 5 + [pl.BlockSpec(memory_space=pl.ANY)],
        out_specs=(vmem,) * 5,
        scratch_shapes=[
            pltpu.VMEM((2, 8, 4, 4, 16, 1024), BF16),
            pltpu.VMEM((256, 256), BF16),
            pltpu.VMEM((4, 80, 256), BF16),
            pltpu.VMEM((8, 2, 80, 256), BF16),
            pltpu.VMEM((8, 128, 256), F32),
            pltpu.VMEM((8, 128, 256), F32),
            pltpu.VMEM((128, 2048), BF16),
            pltpu.VMEM((5, 8, 256), F32),
            pltpu.VMEM((ITERS, 16, 16, 256), F32),
            pltpu.VMEM((ITERS, 4, 16, 256), F32),
            pltpu.VMEM((4, 64, 256), F32),
            dma((32,)),
            dma((8,)), dma((8,)),
            dma((8, 4)), dma((8, 4)),
            dma((8, 4)), dma((8, 4)),
            dma((8,)), dma((8,)),
            dma((16,)), dma((16,)),
            dma((16,)), dma((ITERS, 16)),
            dma((3,)), dma((ITERS, 3)),
            dma((8,)), dma((8,)),
        ],
        compiler_params=pltpu.CompilerParams(
            collective_id=0, has_side_effects=True, vmem_limit_bytes=60 * 2**20
        ),
        name="admm",
    )(
        linear_cost,
        agent_type.reshape(1, -1),
        block_mask.T,
        cost_weight.reshape(1, -1),
        target.reshape(1, -1),
        inverses,
    )
    return usage, shared.reshape(-1), prices.reshape(-1), primal[0, :ITERS], dual[0, :ITERS]


def solution(mesh):
    placed = (
        P("agent", "res"),
        P("agent"),
        P("agent", "res"),
        P(None, "res", None),
        P("res"),
        P("res"),
    )
    return jax.shard_map(
        on_device,
        mesh=mesh,
        in_specs=placed,
        out_specs=(P("agent", "res"), P("res"), P("res"), P(), P()),
        check_vma=False,
    )
```

```python
import functools

import jax
import jax.numpy as jnp
from jax import lax
from jax.experimental import pallas as pl
from jax.experimental.pallas import tpu as pltpu
from jax.sharding import PartitionSpec as P

ITERS = 5
AGENTS = 8192
EPS = 1e-06
MESH = pl.DeviceIdType.MESH
F32 = jnp.float32
BF16 = jnp.bfloat16


def three_parts(value):
    high = value.astype(BF16).astype(F32)
    rest = value - high
    mid = rest.astype(BF16).astype(F32)
    return high, mid, rest - mid


def kernel(
    cost_ref, type_ref, mask_ref, weight_ref, target_ref, inv_ref,
    usage_out, small_out,
    mats, order, packed, rows, expand, usage, others, rhs, shift, vectors, plane, lines, back,
    mat_load, z_send, z_recv, one_send, one_recv, two_send, two_recv, core_send, core_recv,
    row_send, row_recv, hand_send, hand_recv, plane_send, plane_recv, line_send, line_recv, back_send, back_recv,
):
    agent, z = lax.axis_index("agent"), lax.axis_index("res")
    x, y, c = agent // 8, (agent // 2) % 4, agent % 2
    kind = z % 4
    first, second = x * (1 - c) + y * c, y * (1 - c) + x * c
    place = x * 4 + y

    def at(px, py, pc, pz):
        return (px * 8 + py * 2 + pc, pz)

    def along(step_one, step_two):
        one, two = (first + step_one) % 4, (second + step_two) % 4
        return at(one * (1 - c) + two * c, two * (1 - c) + one * c, c, z)

    def copy(src, dst, send, recv, device):
        return pltpu.make_async_remote_copy(src, dst, send, recv, device_id=device, device_id_type=MESH)

    def plane_peer(e):
        other = (place + e) % 16
        return at(other // 4, other % 4, c, z)

    barrier = pltpu.get_barrier_semaphore()

    def greet(e, carry):
        pl.semaphore_signal(barrier, inc=1, device_id=plane_peer(e), device_id_type=MESH)
        return carry

    lax.fori_loop(1, 16, greet, 0)
    for d in range(1, 8):
        pl.semaphore_signal(barrier, inc=1, device_id=at(x, y, c, (z + d) % 8), device_id_type=MESH)
    pl.semaphore_signal(barrier, inc=1, device_id=at(x, y, 1 - c, z), device_id_type=MESH)
    own_loads = [
        pltpu.make_async_copy(
            inv_ref.at[kind, pl.ds(q * 16, 16), pl.ds(h * 1024, 1024)],
            mats.at[h, z, q // 4, q % 4],
            mat_load.at[h * 16 + q],
        )
        for h in range(2)
        for q in range(16)
    ]
    for load in own_loads:
        load.start()
    pl.semaphore_wait(barrier, 23)

    def z_copy(d):
        far = (z + d) % 8
        return copy(
            inv_ref.at[far % 4, pl.ds((first * 4 + second) * 16, 16), pl.ds(pl.multiple_of(c * 1024, 1024), 1024)],
            mats.at[c, z, first, second],
            z_send.at[d],
            z_recv.at[d],
            at(x, y, c, far),
        )

    for d in (4, 3, 5, 2, 6, 1, 7):
        z_copy(d).start()

    kinds = type_ref[...]
    is_kind = (lax.broadcasted_iota(jnp.int32, (16, 256), 0) == kinds).astype(F32)
    before = (
        lax.broadcasted_iota(jnp.int32, (256, 256), 0) < lax.broadcasted_iota(jnp.int32, (256, 256), 1)
    ).astype(BF16)
    ahead = jnp.dot(is_kind.astype(BF16), before, preferred_element_type=F32)
    spot = kinds * 64 + jnp.sum(is_kind * ahead, axis=0, keepdims=True).astype(jnp.int32)
    order[...] = (lax.broadcasted_iota(jnp.int32, (256, 256), 0) == spot).astype(F32).astype(BF16)
    cost = jnp.dot(order[...], cost_ref[...].astype(BF16), preferred_element_type=F32).astype(BF16)
    extra = jnp.concatenate(
        [mask_ref[...].astype(F32), jnp.zeros((14, 256), F32)], axis=0
    ).astype(BF16)
    masks = lax.dot_general(extra, order[...], (((1,), (1,)), ((), ())), preferred_element_type=F32)
    line = lax.broadcasted_iota(jnp.int32, (16, 256), 0)
    lane = lax.broadcasted_iota(jnp.int32, (16, 256), 1)
    tail = jnp.zeros((16, 256), F32)
    for r, part in enumerate(three_parts(weight_ref[...]) + three_parts(target_ref[...])):
        tail = jnp.where(line == 2 + r, part, tail)
    for t in range(4):
        packed[t, :64] = cost[t * 64 : (t + 1) * 64]
        turned = masks if t == 0 else pltpu.roll(masks, 256 - 64 * t, 1)
        packed[t, 64:] = jnp.where((line < 2) & (lane < 64), turned, tail).astype(BF16)

    def row_copy(d):
        far = (z + d) % 8
        return copy(packed.at[far % 4], rows.at[z, c], row_send.at[d], row_recv.at[d], at(x, y, c, far))

    def hand_copy(d):
        block = rows.at[(z - d + 8) % 8, c]
        return copy(block, block, hand_send.at[d], hand_recv.at[d], at(x, y, 1 - c, z))

    for d in (4, 3, 5, 2, 6, 1, 7):
        row_copy(d).start()
    rows[z, c] = packed[kind]
    hand_copy(0).start()

    def part(d):
        return mats.at[c, (z - d + 8) % 8]

    def one_copy(d, s):
        block = part(d).at[first, second]
        return copy(block, block, one_send.at[d, s], one_recv.at[d, s], along(s, 0))

    def two_copy(d, s):
        block = part(d).at[:, second]
        return copy(block, block, two_send.at[d, s], two_recv.at[d, s], along(0, s))

    def core_copy(d):
        return copy(part(d), part(d), core_send.at[d], core_recv.at[d], at(x, y, 1 - c, z))

    for d in (1, 7, 2, 6, 3, 5, 4):
        z_copy(d).wait_recv()
        for s in (2, 1, 3):
            one_copy(d, s).start()
    for d in (1, 7, 2, 6, 3, 5, 4):
        for s in (2, 1, 3):
            one_copy(d, s).wait_recv()
        for s in (2, 1, 3):
            two_copy(d, s).start()
    for d in (1, 7, 2, 6, 3, 5, 4):
        row_copy(d).wait_recv()
        hand_copy(d).start()

    for d in range(8):
        hand_copy(d).wait_recv()
    wide = (lax.broadcasted_iota(jnp.int32, (16, 256), 1) // 128 == line).astype(F32).astype(BF16)
    for j in range(8):
        ends = rows[j, 0, 64:].astype(F32)
        vectors[0, j : j + 1] = ends[2:3] + ends[3:4] + ends[4:5]
        vectors[1, j : j + 1] = ends[5:6] + ends[6:7] + ends[7:8]
        for half in range(2):
            here = rows[j, half, 64:, :128]
            spread = lax.dot_general(here, wide, (((0,), (0,)), ((), ())), preferred_element_type=F32)
            expand[j, half * 64 : half * 64 + 64] = spread[:64]

    for d in (1, 7, 2, 6, 3, 5, 4):
        for s in (2, 1, 3):
            two_copy(d, s).wait_recv()
        core_copy(d).start()
    for load in own_loads:
        load.wait()
    for d in (1, 7, 2, 6, 3, 5, 4):
        core_copy(d).wait_recv()

    norm_lane = lax.broadcasted_iota(jnp.int32, (1, 128), 1)

    def back_copy(e):
        far = (z + e) % 8
        return copy(
            usage.at[far, pl.ds(pl.multiple_of(c * 64, 64), 64)],
            back.at[kind],
            back_send.at[e],
            back_recv.at[e],
            at(x, y, c, far),
        )

    def place_columns(k, j, value):
        plane[k, place, pl.ds(j, 1)] = jnp.sum(value, axis=0, keepdims=True)

    def plane_copy(k, tall, e):
        block = plane.at[k, place, pl.ds(0, tall)]
        return copy(block, block, plane_send.at[k, e], plane_recv.at[k, e], plane_peer(e))

    def start_plane(k, tall):
        def start(e, carry):
            plane_copy(k, tall, e).start()
            return carry

        lax.fori_loop(1, 16, start, 0)

    def end_plane(k, tall):
        def end(e, carry):
            plane_copy(k, tall, e).wait_recv()
            return carry

        lax.fori_loop(1, 16, end, 0)
        return jnp.sum(plane[k, :, :tall], axis=0)

    def line_copy(k, tall, e):
        block = lines.at[k, kind, pl.ds(0, tall)]
        return copy(block, block, line_send.at[k, e], line_recv.at[k, e], at(x, y, c, (z + (1, 7, 2)[e]) % 8))

    def start_line(k, value):
        tall = value.shape[0]
        lines[k, kind, :tall] = value
        for e in range(3):
            line_copy(k, tall, e).start()

    def end_line(k, tall):
        for e in range(3):
            line_copy(k, tall, e).wait_recv()
        return jnp.sum(lines[k, :, :tall], axis=0)

    def block_of(j):
        return mats[j // 4, :, :, :, :, pl.ds(pl.multiple_of((j % 4) * 256, 256), 256)].reshape(2048, 256)

    def lanes_of(j):
        return pl.ds(pl.multiple_of(j * 256, 256), 256)

    def costs_of(j):
        return rows[j, :, :64].astype(F32).reshape(128, 256)

    def product(j):
        return jnp.dot(rhs[...], block_of(j), preferred_element_type=F32)

    def applied(k, summed=True):
        def step(j, carry):
            fresh = product(j)
            others[j] = fresh
            if summed:
                place_columns(k, j, fresh * expand[j])
            return carry

        lax.fori_loop(0, 8, step, 0)

    def common(v):
        high, mid, low = three_parts(v)
        for j in range(8):
            stack = jnp.where(line == 0, high[j : j + 1], jnp.where(line == 1, mid[j : j + 1], low[j : j + 1]))
            shift[:, j * 256 : (j + 1) * 256] = jnp.where(line < 3, stack, 0.0).astype(BF16)

        def step(j, carry):
            out = jnp.dot(shift[...], block_of(j), preferred_element_type=F32)
            vectors[4, pl.ds(j, 1)] = out[0:1] + out[1:2] + out[2:3]
            return carry

        lax.fori_loop(0, 8, step, 0)
        return vectors[4]

    def advance(k, last=False):
        def step(j, change):
            fresh = (others[j] + vectors[4, pl.ds(j, 1)]) * expand[j]
            gap = fresh - usage[j]
            usage[j] = fresh
            if last:
                place_columns(4, j, fresh)
            else:
                rhs[:, lanes_of(j)] = (fresh - costs_of(j)).astype(BF16)
            return change + jnp.sum(gap * gap, axis=0, keepdims=True)

        change = lax.fori_loop(0, 8, step, jnp.zeros((1, 256), F32))
        plane[4, place, 7 + k : 8 + k] = change

    def settle(total, prices, norms, k):
        mean = total * (1.0 / AGENTS)
        shared = (vectors[0] * vectors[1] + (prices + mean)) / (vectors[0] + 1.0)
        prices = prices + mean - shared
        gap = mean - shared
        norms = jnp.where(norm_lane == k - 1, float(AGENTS) * jnp.sum(gap * gap), norms)
        return shared - mean - prices, shared, prices, norms

    def negated(j, carry):
        rhs[:, lanes_of(j)] = -rows[j, :, :64].reshape(128, 256)
        return carry

    lax.fori_loop(0, 8, negated, 0)

    def opening(j, change):
        fresh = product(j) * expand[j]
        usage[j] = fresh
        place_columns(0, j, fresh)
        return change + jnp.sum(fresh * fresh, axis=0, keepdims=True)

    change = lax.fori_loop(0, 8, opening, jnp.zeros((1, 256), F32))
    plane[4, place, 8:9] = change
    for j in range(8):
        plane[0, place, 8 + j : 9 + j] = jnp.sum(expand[j], axis=0, keepdims=True)
    start_plane(0, 16)

    def second_side(j, carry):
        rhs[:, lanes_of(j)] = (usage[j] - costs_of(j)).astype(BF16)
        return carry

    lax.fori_loop(0, 8, second_side, 0)
    applied(1)
    start_plane(1, 8)
    sums = end_plane(0, 16)
    start_line(0, sums[:8])
    counts = sums[8:]
    start_line(1, end_plane(1, 8))
    norms = jnp.zeros((1, 128), F32)
    v, shared, prices, norms = settle(end_line(0, 8), jnp.zeros((8, 256), F32), norms, 1)

    start_line(5, counts * common(v))
    advance(2)
    applied(2)
    start_plane(2, 8)
    v, shared, prices, norms = settle(end_line(1, 8) + end_line(5, 8), prices, norms, 2)

    start_line(6, counts * common(v))
    advance(3)
    applied(3)
    start_plane(3, 8)
    start_line(2, end_plane(2, 8))
    v, shared, prices, norms = settle(end_line(2, 8) + end_line(6, 8), prices, norms, 3)

    start_line(7, counts * common(v))
    start_line(3, end_plane(3, 8))
    advance(4)
    applied(4, summed=False)
    v, shared, prices, norms = settle(end_line(3, 8) + end_line(7, 8), prices, norms, 4)

    common(v)
    advance(5, last=True)
    for e in (1, 7, 2):
        back_copy(e).start()
    plane[4, place, 13:] = jnp.zeros((3, 256), F32)
    start_plane(4, 16)
    back[kind] = usage[z, pl.ds(pl.multiple_of(c * 64, 64), 64)]
    start_line(4, end_plane(4, 16))
    for e in (1, 7, 2):
        back_copy(e).wait_recv()
    result = jnp.zeros((256, 256), F32)
    for piece in three_parts(back[...].reshape(256, 256)):
        result += lax.dot_general(
            order[...], piece.astype(BF16), (((0,), (0,)), ((), ())), preferred_element_type=F32
        )
    usage_out[...] = result
    total = end_line(4, 16)
    v, shared, prices, norms = settle(total[:8], prices, norms, 5)
    duals = jnp.zeros((1, 128), F32)
    for k in range(ITERS):
        duals = jnp.where(norm_lane == k, jnp.sum(total[8 + k : 9 + k]), duals)
    vectors[2] = shared
    vectors[3] = prices
    small_out[0:1] = vectors[2, pl.ds(z, 1)]
    small_out[1:2] = vectors[3, pl.ds(z, 1)]
    small_out[2:3, :128] = jnp.sqrt(norms + EPS)
    small_out[3:4, :128] = jnp.sqrt(duals + EPS)

    def end_sends(e, carry):
        for k, tall in enumerate((16, 8, 8, 8, 16)):
            plane_copy(k, tall, e).wait_send()
        return carry

    lax.fori_loop(1, 16, end_sends, 0)
    for k, tall in enumerate((8, 8, 8, 8, 16, 8, 8, 8)):
        for e in range(3):
            line_copy(k, tall, e).wait_send()
    for d in range(8):
        hand_copy(d).wait_send()
    for d in range(1, 8):
        row_copy(d).wait_send()
        z_copy(d).wait_send()
        for s in (1, 2, 3):
            one_copy(d, s).wait_send()
            two_copy(d, s).wait_send()
        core_copy(d).wait_send()
    for e in (1, 7, 2):
        back_copy(e).wait_send()


def on_device(linear_cost, agent_type, block_mask, inverses, cost_weight, target):
    vmem = pl.BlockSpec(memory_space=pltpu.VMEM)
    dma = pltpu.SemaphoreType.DMA
    usage, small = pl.pallas_call(
        kernel,
        out_shape=(jax.ShapeDtypeStruct((256, 256), F32), jax.ShapeDtypeStruct((4, 256), F32)),
        in_specs=[vmem] * 5 + [pl.BlockSpec(memory_space=pl.ANY)],
        out_specs=(vmem,) * 2,
        scratch_shapes=[
            pltpu.VMEM((2, 8, 4, 4, 16, 1024), BF16),
            pltpu.VMEM((256, 256), BF16),
            pltpu.VMEM((4, 80, 256), BF16),
            pltpu.VMEM((8, 2, 80, 256), BF16),
            pltpu.VMEM((8, 128, 256), F32),
            pltpu.VMEM((8, 128, 256), F32),
            pltpu.VMEM((8, 128, 256), F32),
            pltpu.VMEM((128, 2048), BF16),
            pltpu.VMEM((16, 2048), BF16),
            pltpu.VMEM((5, 8, 256), F32),
            pltpu.VMEM((ITERS, 16, 16, 256), F32),
            pltpu.VMEM((8, 4, 16, 256), F32),
            pltpu.VMEM((4, 64, 256), F32),
            dma((32,)),
            dma((8,)), dma((8,)),
            dma((8, 4)), dma((8, 4)),
            dma((8, 4)), dma((8, 4)),
            dma((8,)), dma((8,)),
            dma((8,)), dma((8,)),
            dma((8,)), dma((8,)),
            dma((ITERS, 16)), dma((ITERS, 16)),
            dma((8, 3)), dma((8, 3)),
            dma((8,)), dma((8,)),
        ],
        compiler_params=pltpu.CompilerParams(
            collective_id=0, has_side_effects=True, vmem_limit_bytes=60 * 2**20
        ),
        name="admm",
    )(
        linear_cost,
        agent_type.reshape(1, -1),
        block_mask.T,
        cost_weight.reshape(1, -1),
        target.reshape(1, -1),
        inverses,
    )
    return usage, small[0], small[1], small[2, :ITERS], small[3, :ITERS]


def solution(mesh):
    placed = (
        P("agent", "res"),
        P("agent"),
        P("agent", "res"),
        P(None, "res", None),
        P("res"),
        P("res"),
    )
    return jax.shard_map(
        on_device,
        mesh=mesh,
        in_specs=placed,
        out_specs=(P("agent", "res"), P("res"), P("res"), P(), P()),
        check_vma=False,
    )
```

```python
import functools

import jax
import jax.numpy as jnp
from jax import lax
from jax.experimental import pallas as pl
from jax.experimental.pallas import tpu as pltpu
from jax.sharding import PartitionSpec as P

ITERS = 5
AGENTS = 8192
EPS = 1e-06
MESH = pl.DeviceIdType.MESH
F32 = jnp.float32
BF16 = jnp.bfloat16


def three_parts(value):
    high = value.astype(BF16).astype(F32)
    rest = value - high
    mid = rest.astype(BF16).astype(F32)
    return high, mid, rest - mid


def kernel(
    cost_ref, type_ref, mask_ref, weight_ref, target_ref, inv_ref,
    usage_out, small_out,
    stage, half, full, order, packed, rows, expand, usage, others, rhs, shift, vectors, plane, lines, back,
    stage_load, mat_load, z_send, z_recv, one_send, one_recv, two_send, two_recv, core_send, core_recv,
    row_send, row_recv, hand_send, hand_recv, plane_send, plane_recv, line_send, line_recv, back_send, back_recv,
):
    agent, z = lax.axis_index("agent"), lax.axis_index("res")
    x, y, c = agent // 8, (agent // 2) % 4, agent % 2
    kind = z % 4
    first, second = x * (1 - c) + y * c, y * (1 - c) + x * c
    place = x * 4 + y

    def at(px, py, pc, pz):
        return (px * 8 + py * 2 + pc, pz)

    def along(step_one, step_two):
        one, two = (first + step_one) % 4, (second + step_two) % 4
        return at(one * (1 - c) + two * c, two * (1 - c) + one * c, c, z)

    def copy(src, dst, send, recv, device):
        return pltpu.make_async_remote_copy(src, dst, send, recv, device_id=device, device_id_type=MESH)

    def plane_peer(e):
        other = (place + e) % 16
        return at(other // 4, other % 4, c, z)

    barrier = pltpu.get_barrier_semaphore()

    def greet(e, carry):
        pl.semaphore_signal(barrier, inc=1, device_id=plane_peer(e), device_id_type=MESH)
        return carry

    lax.fori_loop(1, 16, greet, 0)
    for d in range(1, 8):
        pl.semaphore_signal(barrier, inc=1, device_id=at(x, y, c, (z + d) % 8), device_id_type=MESH)
    pl.semaphore_signal(barrier, inc=1, device_id=at(x, y, 1 - c, z), device_id_type=MESH)
    def column(k):
        return pl.ds(pl.multiple_of(((2 * z + k) % 16) * 128, 128), 128)

    own_loads = [
        pltpu.make_async_copy(
            inv_ref.at[t, first, second, :, column(c * 5 + i)],
            stage.at[t, :, pl.ds(i * 128, 128)],
            stage_load.at[t * 5 + i],
        )
        for t in range(4)
        for i in range(5)
    ] + [
        pltpu.make_async_copy(
            inv_ref.at[kind, :, :, :, column(k)],
            half.at[k // 5, z, :, :, :, pl.ds((k % 5) * 128, 128)],
            mat_load.at[k],
        )
        for k in range(10)
    ]
    for load in own_loads:
        load.start()
    for load in own_loads[:20]:
        load.wait()
    pl.semaphore_wait(barrier, 23)

    def z_copy(d):
        far = (z + d) % 8
        return copy(
            stage.at[far % 4], half.at[c, z, first, second], z_send.at[d], z_recv.at[d], at(x, y, c, far)
        )

    for d in (4, 3, 5, 2, 6, 1, 7):
        z_copy(d).start()

    kinds = type_ref[...]
    is_kind = (lax.broadcasted_iota(jnp.int32, (16, 256), 0) == kinds).astype(F32)
    before = (
        lax.broadcasted_iota(jnp.int32, (256, 256), 0) < lax.broadcasted_iota(jnp.int32, (256, 256), 1)
    ).astype(BF16)
    ahead = jnp.dot(is_kind.astype(BF16), before, preferred_element_type=F32)
    spot = kinds * 64 + jnp.sum(is_kind * ahead, axis=0, keepdims=True).astype(jnp.int32)
    order[...] = (lax.broadcasted_iota(jnp.int32, (256, 256), 0) == spot).astype(F32).astype(BF16)
    cost = jnp.dot(order[...], cost_ref[...].astype(BF16), preferred_element_type=F32).astype(BF16)
    extra = jnp.concatenate(
        [mask_ref[...].astype(F32), jnp.zeros((14, 256), F32)], axis=0
    ).astype(BF16)
    masks = lax.dot_general(extra, order[...], (((1,), (1,)), ((), ())), preferred_element_type=F32)
    line = lax.broadcasted_iota(jnp.int32, (16, 256), 0)
    lane = lax.broadcasted_iota(jnp.int32, (16, 256), 1)
    tail = jnp.zeros((16, 256), F32)
    for r, part in enumerate(three_parts(weight_ref[...]) + three_parts(target_ref[...])):
        tail = jnp.where(line == 2 + r, part, tail)
    for t in range(4):
        packed[t, :64] = cost[t * 64 : (t + 1) * 64]
        turned = masks if t == 0 else pltpu.roll(masks, 256 - 64 * t, 1)
        packed[t, 64:] = jnp.where((line < 2) & (lane < 64), turned, tail).astype(BF16)

    def row_copy(d):
        far = (z + d) % 8
        return copy(packed.at[far % 4], rows.at[z, c], row_send.at[d], row_recv.at[d], at(x, y, c, far))

    def hand_copy(d):
        block = rows.at[(z - d + 8) % 8, c]
        return copy(block, block, hand_send.at[d], hand_recv.at[d], at(x, y, 1 - c, z))

    for d in (4, 3, 5, 2, 6, 1, 7):
        row_copy(d).start()
    rows[z, c] = packed[kind]
    hand_copy(0).start()

    def part(d):
        return half.at[c, (z - d + 8) % 8]

    def one_copy(d, s):
        block = part(d).at[first, second]
        return copy(block, block, one_send.at[d, s], one_recv.at[d, s], along(s, 0))

    def two_copy(d, s):
        block = part(d).at[:, second]
        return copy(block, block, two_send.at[d, s], two_recv.at[d, s], along(0, s))

    def core_copy(d):
        return copy(part(d), part(d), core_send.at[d], core_recv.at[d], at(x, y, 1 - c, z))

    for d in (1, 7, 2, 6, 3, 5, 4):
        z_copy(d).wait_recv()
        for s in (2, 1, 3):
            one_copy(d, s).start()
    for d in (1, 7, 2, 6, 3, 5, 4):
        for s in (2, 1, 3):
            one_copy(d, s).wait_recv()
        for s in (2, 1, 3):
            two_copy(d, s).start()
    for d in (1, 7, 2, 6, 3, 5, 4):
        row_copy(d).wait_recv()
        hand_copy(d).start()

    for d in range(8):
        hand_copy(d).wait_recv()
    wide = (lax.broadcasted_iota(jnp.int32, (16, 256), 1) // 128 == line).astype(F32).astype(BF16)
    for j in range(8):
        ends = rows[j, 0, 64:].astype(F32)
        vectors[0, j : j + 1] = ends[2:3] + ends[3:4] + ends[4:5]
        vectors[1, j : j + 1] = ends[5:6] + ends[6:7] + ends[7:8]
        for side in range(2):
            here = rows[j, side, 64:, :128]
            spread = lax.dot_general(here, wide, (((0,), (0,)), ((), ())), preferred_element_type=F32)
            expand[j, side * 64 : side * 64 + 64] = spread[:64]

    def fill(block):
        for k in range(10):
            tile = half[k // 5, block, :, :, :, (k % 5) * 128 : (k % 5) * 128 + 128].reshape(256, 128)
            across = (block + k // 2) % 8
            full[across, pl.ds(pl.multiple_of(block * 256, 256), 256), (k % 2) * 128 : (k % 2) * 128 + 128] = tile
            if 2 <= k < 8:
                full[block, pl.ds(pl.multiple_of(across * 256 + (k % 2) * 128, 128), 128), :] = tile.T

    for load in own_loads[20:]:
        load.wait()
    fill(z)
    ahead_of = 0
    for d in (1, 7, 2, 6, 3, 5, 4, 0):
        if d:
            for s in (2, 1, 3):
                two_copy(d, s).wait_recv()
            core_copy(d).start()
        if ahead_of:
            core_copy(ahead_of).wait_recv()
            fill((z - ahead_of + 8) % 8)
        ahead_of = d

    norm_lane = lax.broadcasted_iota(jnp.int32, (1, 128), 1)

    def back_copy(e):
        far = (z + e) % 8
        return copy(
            usage.at[far, pl.ds(pl.multiple_of(c * 64, 64), 64)],
            back.at[kind],
            back_send.at[e],
            back_recv.at[e],
            at(x, y, c, far),
        )

    def place_columns(k, j, value):
        plane[k, place, pl.ds(j, 1)] = jnp.sum(value, axis=0, keepdims=True)

    def plane_copy(k, tall, e):
        block = plane.at[k, place, pl.ds(0, tall)]
        return copy(block, block, plane_send.at[k, e], plane_recv.at[k, e], plane_peer(e))

    def start_plane(k, tall):
        def start(e, carry):
            plane_copy(k, tall, e).start()
            return carry

        lax.fori_loop(1, 16, start, 0)

    def end_plane(k, tall):
        def end(e, carry):
            plane_copy(k, tall, e).wait_recv()
            return carry

        lax.fori_loop(1, 16, end, 0)
        return jnp.sum(plane[k, :, :tall], axis=0)

    def line_copy(k, tall, e):
        block = lines.at[k, kind, pl.ds(0, tall)]
        return copy(block, block, line_send.at[k, e], line_recv.at[k, e], at(x, y, c, (z + (1, 7, 2)[e]) % 8))

    def start_line(k, value):
        tall = value.shape[0]
        lines[k, kind, :tall] = value
        for e in range(3):
            line_copy(k, tall, e).start()

    def end_line(k, tall):
        for e in range(3):
            line_copy(k, tall, e).wait_recv()
        return jnp.sum(lines[k, :, :tall], axis=0)

    def block_of(j):
        return full[j]

    def lanes_of(j):
        return pl.ds(pl.multiple_of(j * 256, 256), 256)

    def costs_of(j):
        return rows[j, :, :64].astype(F32).reshape(128, 256)

    def product(j):
        return jnp.dot(rhs[...], block_of(j), preferred_element_type=F32)

    def applied(k):
        def step(j, carry):
            fresh = product(j)
            others[j] = fresh
            place_columns(k, j, fresh * expand[j])
            return carry

        lax.fori_loop(0, 8, step, 0)

    def common(v):
        high, mid, low = three_parts(v)
        for j in range(8):
            stack = jnp.where(line == 0, high[j : j + 1], jnp.where(line == 1, mid[j : j + 1], low[j : j + 1]))
            shift[:, j * 256 : (j + 1) * 256] = jnp.where(line < 3, stack, 0.0).astype(BF16)

        def step(j, carry):
            out = jnp.dot(shift[...], block_of(j), preferred_element_type=F32)
            vectors[4, pl.ds(j, 1)] = out[0:1] + out[1:2] + out[2:3]
            return carry

        lax.fori_loop(0, 8, step, 0)
        return vectors[4]

    def advance(k):
        def step(j, change):
            fresh = (others[j] + vectors[4, pl.ds(j, 1)]) * expand[j]
            gap = fresh - usage[j]
            usage[j] = fresh
            rhs[:, lanes_of(j)] = (fresh - costs_of(j)).astype(BF16)
            return change + jnp.sum(gap * gap, axis=0, keepdims=True)

        change = lax.fori_loop(0, 8, step, jnp.zeros((1, 256), F32))
        plane[4, place, 7 + k : 8 + k] = change

    def settle(total, prices, norms, k):
        mean = total * (1.0 / AGENTS)
        shared = (vectors[0] * vectors[1] + (prices + mean)) / (vectors[0] + 1.0)
        prices = prices + mean - shared
        gap = mean - shared
        norms = jnp.where(norm_lane == k - 1, float(AGENTS) * jnp.sum(gap * gap), norms)
        return shared - mean - prices, shared, prices, norms

    def negated(j, carry):
        rhs[:, lanes_of(j)] = -rows[j, :, :64].reshape(128, 256)
        return carry

    lax.fori_loop(0, 8, negated, 0)

    def opening(j, change):
        fresh = product(j) * expand[j]
        usage[j] = fresh
        place_columns(0, j, fresh)
        return change + jnp.sum(fresh * fresh, axis=0, keepdims=True)

    change = lax.fori_loop(0, 8, opening, jnp.zeros((1, 256), F32))
    plane[4, place, 8:9] = change
    for j in range(8):
        plane[0, place, 8 + j : 9 + j] = jnp.sum(expand[j], axis=0, keepdims=True)
    start_plane(0, 16)

    def second_side(j, carry):
        rhs[:, lanes_of(j)] = (usage[j] - costs_of(j)).astype(BF16)
        return carry

    lax.fori_loop(0, 8, second_side, 0)
    applied(1)
    start_plane(1, 8)
    sums = end_plane(0, 16)
    start_line(0, sums[:8])
    counts = sums[8:]
    start_line(1, end_plane(1, 8))
    norms = jnp.zeros((1, 128), F32)
    v, shared, prices, norms = settle(end_line(0, 8), jnp.zeros((8, 256), F32), norms, 1)

    start_line(5, counts * common(v))
    advance(2)
    applied(2)
    start_plane(2, 8)
    v, shared, prices, norms = settle(end_line(1, 8) + end_line(5, 8), prices, norms, 2)

    start_line(6, counts * common(v))
    advance(3)
    applied(3)
    start_plane(3, 8)
    start_line(2, end_plane(2, 8))
    v, shared, prices, norms = settle(end_line(2, 8) + end_line(6, 8), prices, norms, 3)

    start_line(7, counts * common(v))
    start_line(3, end_plane(3, 8))
    advance(4)
    v, shared, prices, norms = settle(end_line(3, 8) + end_line(7, 8), prices, norms, 4)

    vectors[4] = v

    def last_side(j, carry):
        rhs[:, lanes_of(j)] = (usage[j] + vectors[4, pl.ds(j, 1)] - costs_of(j)).astype(BF16)
        return carry

    def closing(j, change):
        fresh = product(j) * expand[j]
        gap = fresh - usage[j]
        usage[j] = fresh
        place_columns(4, j, fresh)
        return change + jnp.sum(gap * gap, axis=0, keepdims=True)

    lax.fori_loop(0, 8, last_side, 0)
    plane[4, place, 12:13] = lax.fori_loop(0, 8, closing, jnp.zeros((1, 256), F32))
    for e in (1, 7, 2):
        back_copy(e).start()
    plane[4, place, 13:] = jnp.zeros((3, 256), F32)
    start_plane(4, 16)
    back[kind] = usage[z, pl.ds(pl.multiple_of(c * 64, 64), 64)]
    start_line(4, end_plane(4, 16))
    for e in (1, 7, 2):
        back_copy(e).wait_recv()
    result = jnp.zeros((256, 256), F32)
    for piece in three_parts(back[...].reshape(256, 256)):
        result += lax.dot_general(
            order[...], piece.astype(BF16), (((0,), (0,)), ((), ())), preferred_element_type=F32
        )
    usage_out[...] = result
    total = end_line(4, 16)
    v, shared, prices, norms = settle(total[:8], prices, norms, 5)
    duals = jnp.zeros((1, 128), F32)
    for k in range(ITERS):
        duals = jnp.where(norm_lane == k, jnp.sum(total[8 + k : 9 + k]), duals)
    vectors[2] = shared
    vectors[3] = prices
    small_out[0:1] = vectors[2, pl.ds(z, 1)]
    small_out[1:2] = vectors[3, pl.ds(z, 1)]
    small_out[2:3, :128] = jnp.sqrt(norms + EPS)
    small_out[3:4, :128] = jnp.sqrt(duals + EPS)

    def end_sends(e, carry):
        for k, tall in enumerate((16, 8, 8, 8, 16)):
            plane_copy(k, tall, e).wait_send()
        return carry

    lax.fori_loop(1, 16, end_sends, 0)
    for k, tall in enumerate((8, 8, 8, 8, 16, 8, 8, 8)):
        for e in range(3):
            line_copy(k, tall, e).wait_send()
    for d in range(8):
        hand_copy(d).wait_send()
    for d in range(1, 8):
        row_copy(d).wait_send()
        z_copy(d).wait_send()
        for s in (1, 2, 3):
            one_copy(d, s).wait_send()
            two_copy(d, s).wait_send()
        core_copy(d).wait_send()
    for e in (1, 7, 2):
        back_copy(e).wait_send()


def on_device(linear_cost, agent_type, block_mask, inverses, cost_weight, target):
    vmem = pl.BlockSpec(memory_space=pltpu.VMEM)
    dma = pltpu.SemaphoreType.DMA
    usage, small = pl.pallas_call(
        kernel,
        out_shape=(jax.ShapeDtypeStruct((256, 256), F32), jax.ShapeDtypeStruct((4, 256), F32)),
        in_specs=[vmem] * 5 + [pl.BlockSpec(memory_space=pl.ANY)],
        out_specs=(vmem,) * 2,
        scratch_shapes=[
            pltpu.VMEM((4, 16, 640), BF16),
            pltpu.VMEM((2, 8, 4, 4, 16, 640), BF16),
            pltpu.VMEM((8, 2048, 256), BF16),
            pltpu.VMEM((256, 256), BF16),
            pltpu.VMEM((4, 80, 256), BF16),
            pltpu.VMEM((8, 2, 80, 256), BF16),
            pltpu.VMEM((8, 128, 256), F32),
            pltpu.VMEM((8, 128, 256), F32),
            pltpu.VMEM((8, 128, 256), F32),
            pltpu.VMEM((128, 2048), BF16),
            pltpu.VMEM((16, 2048), BF16),
            pltpu.VMEM((5, 8, 256), F32),
            pltpu.VMEM((ITERS, 16, 16, 256), F32),
            pltpu.VMEM((8, 4, 16, 256), F32),
            pltpu.VMEM((4, 64, 256), F32),
            dma((20,)), dma((10,)),
            dma((8,)), dma((8,)),
            dma((8, 4)), dma((8, 4)),
            dma((8, 4)), dma((8, 4)),
            dma((8,)), dma((8,)),
            dma((8,)), dma((8,)),
            dma((8,)), dma((8,)),
            dma((ITERS, 16)), dma((ITERS, 16)),
            dma((8, 3)), dma((8, 3)),
            dma((8,)), dma((8,)),
        ],
        compiler_params=pltpu.CompilerParams(
            collective_id=0, has_side_effects=True, vmem_limit_bytes=60 * 2**20
        ),
        name="admm",
    )(
        linear_cost,
        agent_type.reshape(1, -1),
        block_mask.T,
        cost_weight.reshape(1, -1),
        target.reshape(1, -1),
        inverses.reshape(4, 4, 4, 16, 2048),
    )
    return usage, small[0], small[1], small[2, :ITERS], small[3, :ITERS]


def solution(mesh):
    placed = (
        P("agent", "res"),
        P("agent"),
        P("agent", "res"),
        P(None, "res", None),
        P("res"),
        P("res"),
    )
    return jax.shard_map(
        on_device,
        mesh=mesh,
        in_specs=placed,
        out_specs=(P("agent", "res"), P("res"), P("res"), P(), P()),
        check_vma=False,
    )
```

```python
import functools

import jax
import jax.numpy as jnp
from jax import lax
from jax.experimental import pallas as pl
from jax.experimental.pallas import tpu as pltpu
from jax.sharding import PartitionSpec as P

ITERS = 5
LAG_TWO, LAG_THREE, LAG_FOUR = 3, 6, 7
LAST_STEP = LAG_FOUR + 7
AGENTS = 8192
EPS = 1e-06
MESH = pl.DeviceIdType.MESH
F32 = jnp.float32
BF16 = jnp.bfloat16


def three_parts(value):
    high = value.astype(BF16).astype(F32)
    rest = value - high
    mid = rest.astype(BF16).astype(F32)
    return high, mid, rest - mid


def kernel(
    cost_ref, type_ref, mask_ref, weight_ref, target_ref, inv_ref,
    usage_out, small_out,
    stage, half, full, order, packed, rows, expand, usage, rhs, plain, counts, vectors, plane, lines, back,
    stage_load, mat_load, z_send, z_recv, one_send, one_recv, two_send, two_recv, core_send, core_recv,
    row_send, row_recv, hand_send, hand_recv, plane_send, plane_recv, line_send, line_recv, back_send, back_recv,
):
    agent, z = lax.axis_index("agent"), lax.axis_index("res")
    x, y, c = agent // 8, (agent // 2) % 4, agent % 2
    kind = z % 4
    first, second = x * (1 - c) + y * c, y * (1 - c) + x * c
    place = x * 4 + y

    def at(px, py, pc, pz):
        return (px * 8 + py * 2 + pc, pz)

    def along(step_one, step_two):
        one, two = (first + step_one) % 4, (second + step_two) % 4
        return at(one * (1 - c) + two * c, two * (1 - c) + one * c, c, z)

    def copy(src, dst, send, recv, device):
        return pltpu.make_async_remote_copy(src, dst, send, recv, device_id=device, device_id_type=MESH)

    def plane_peer(e):
        other = (place + e) % 16
        return at(other // 4, other % 4, c, z)

    barrier = pltpu.get_barrier_semaphore()

    def greet(e, carry):
        pl.semaphore_signal(barrier, inc=1, device_id=plane_peer(e), device_id_type=MESH)
        return carry

    lax.fori_loop(1, 16, greet, 0)
    for d in range(1, 8):
        pl.semaphore_signal(barrier, inc=1, device_id=at(x, y, c, (z + d) % 8), device_id_type=MESH)
    for d in (0, 1, 7, 2, 6):
        pl.semaphore_signal(barrier, inc=1, device_id=at(x, y, 1 - c, (z + d) % 8), device_id_type=MESH)
    def column(k):
        return pl.ds(pl.multiple_of(((2 * z + k) % 16) * 128, 128), 128)

    own_loads = [
        pltpu.make_async_copy(
            inv_ref.at[t, first, second, :, column(c * 5 + i)],
            stage.at[t, :, pl.ds(i * 128, 128)],
            stage_load.at[t * 5 + i],
        )
        for t in range(4)
        for i in range(5)
    ] + [
        pltpu.make_async_copy(
            inv_ref.at[kind, :, :, :, column(k)],
            half.at[k // 5, z, :, :, :, pl.ds((k % 5) * 128, 128)],
            mat_load.at[k],
        )
        for k in range(10)
    ]
    for load in own_loads:
        load.start()
    def z_copy(d):
        far = (z + d) % 8
        return copy(
            stage.at[far % 4], half.at[c, z, first, second], z_send.at[d], z_recv.at[d], at(x, y, c, far)
        )


    kinds = type_ref[...]
    is_kind = (lax.broadcasted_iota(jnp.int32, (16, 256), 0) == kinds).astype(F32)
    before = (
        lax.broadcasted_iota(jnp.int32, (256, 256), 0) < lax.broadcasted_iota(jnp.int32, (256, 256), 1)
    ).astype(BF16)
    ahead = jnp.dot(is_kind.astype(BF16), before, preferred_element_type=F32)
    spot = kinds * 64 + jnp.sum(is_kind * ahead, axis=0, keepdims=True).astype(jnp.int32)
    order[...] = (lax.broadcasted_iota(jnp.int32, (256, 256), 0) == spot).astype(F32).astype(BF16)
    cost = jnp.dot(order[...], cost_ref[...].astype(BF16), preferred_element_type=F32).astype(BF16)
    extra = jnp.concatenate(
        [mask_ref[...].astype(F32), jnp.zeros((14, 256), F32)], axis=0
    ).astype(BF16)
    masks = lax.dot_general(extra, order[...], (((1,), (1,)), ((), ())), preferred_element_type=F32)
    line = lax.broadcasted_iota(jnp.int32, (16, 256), 0)
    lane = lax.broadcasted_iota(jnp.int32, (16, 256), 1)
    tail = jnp.zeros((16, 256), F32)
    for r, part in enumerate(three_parts(weight_ref[...]) + three_parts(target_ref[...])):
        tail = jnp.where(line == 2 + r, part, tail)
    for t in range(4):
        packed[t, :64] = cost[t * 64 : (t + 1) * 64]
        turned = masks if t == 0 else pltpu.roll(masks, 256 - 64 * t, 1)
        packed[t, 64:] = jnp.where((line < 2) & (lane < 64), turned, tail).astype(BF16)

    def row_copy(d):
        far = (z + d) % 8
        return copy(packed.at[far % 4], rows.at[z, c], row_send.at[d], row_recv.at[d], at(x, y, c, far))

    def hand_copy(d):
        block = rows.at[(z - d + 8) % 8, c]
        return copy(block, block, hand_send.at[d], hand_recv.at[d], at(x, y, 1 - c, z))

    for load in own_loads[:20]:
        load.wait()
    pl.semaphore_wait(barrier, 27)
    for d in (4, 3, 5, 2, 6, 1, 7):
        z_copy(d).start()
    for d in (4, 3, 5, 2, 6, 1, 7):
        row_copy(d).start()
    rows[z, c] = packed[kind]
    hand_copy(0).start()

    def part(d):
        return half.at[c, (z - d + 8) % 8]

    def one_copy(d, s):
        block = part(d).at[first, second]
        return copy(block, block, one_send.at[d, s], one_recv.at[d, s], along(s, 0))

    def two_copy(d, s):
        block = part(d).at[:, second]
        return copy(block, block, two_send.at[d, s], two_recv.at[d, s], along(0, s))

    def core_copy(d):
        return copy(part(d), part(d), core_send.at[d], core_recv.at[d], at(x, y, 1 - c, z))

    line = lax.broadcasted_iota(jnp.int32, (16, 256), 0)
    wide = (lax.broadcasted_iota(jnp.int32, (16, 256), 1) // 128 == line).astype(F32).astype(BF16)

    def fill(block):
        for k in range(10):
            tile = half[k // 5, block, :, :, :, (k % 5) * 128 : (k % 5) * 128 + 128].reshape(256, 128)
            across = (block + k // 2) % 8
            full[across, pl.ds(pl.multiple_of(block * 256, 256), 256), (k % 2) * 128 : (k % 2) * 128 + 128] = tile
            if 2 <= k < 8:
                full[block, pl.ds(pl.multiple_of(across * 256 + (k % 2) * 128, 128), 128), :] = tile.T

    def stage_one(d):
        z_copy(d).wait_recv()
        for s in (2, 1, 3):
            one_copy(d, s).start()

    def stage_two(d):
        for s in (2, 1, 3):
            one_copy(d, s).wait_recv()
        for s in (2, 1, 3):
            two_copy(d, s).start()

    def stage_three(d):
        for s in (2, 1, 3):
            two_copy(d, s).wait_recv()
        core_copy(d).start()

    def stage_four(d):
        core_copy(d).wait_recv()
        fill((z - d + 8) % 8)

    def unpack():
        for d in (1, 7, 2, 6, 3, 5, 4):
            row_copy(d).wait_recv()
            hand_copy(d).start()
        for load in own_loads[20:]:
            load.wait()
        fill(z)
        for d in range(8):
            hand_copy(d).wait_recv()
        for j in range(8):
            ends = rows[j, 0, 64:].astype(F32)
            vectors[0, j : j + 1] = ends[2:3] + ends[3:4] + ends[4:5]
            vectors[1, j : j + 1] = ends[5:6] + ends[6:7] + ends[7:8]
            for side in range(2):
                here = rows[j, side, 64:, :128]
                spread = lax.dot_general(here, wide, (((0,), (0,)), ((), ())), preferred_element_type=F32)
                expand[j, side * 64 : side * 64 + 64] = spread[:64]

    turns = (1, 7, 2, 6, 3, 5, 4)
    for step in range(LAST_STEP):
        for lag, act in ((0, stage_one), (LAG_TWO, stage_two), (LAG_THREE, stage_three), (LAG_FOUR, stage_four)):
            if 0 <= step - lag < 7:
                act(turns[step - lag])
        if step == 8:
            unpack()

    norm_lane = lax.broadcasted_iota(jnp.int32, (1, 128), 1)

    def back_copy(e):
        far = (z + e) % 8
        return copy(
            usage.at[far, pl.ds(pl.multiple_of(c * 64, 64), 64)],
            back.at[kind],
            back_send.at[e],
            back_recv.at[e],
            at(x, y, c, far),
        )

    def place_columns(k, j, value):
        plane[k, place, pl.ds(j, 1)] = jnp.sum(value, axis=0, keepdims=True)

    def plane_copy(k, tall, e):
        block = plane.at[k, place, pl.ds(0, tall)]
        return copy(block, block, plane_send.at[k, e], plane_recv.at[k, e], plane_peer(e))

    def start_plane(k, tall):
        @pl.when(c == 1)
        def _():
            def start(e, carry):
                plane_copy(k, tall, e).start()
                return carry

            lax.fori_loop(1, 16, start, 0)

    def line_copy(k, tall, i):
        e = i // 2
        far = at(x, y, 1 - c, z) if e == 3 else at(x, y, 1 - i % 2, (z + (1, 7, 2)[e]) % 8)
        block = lines.at[k, kind, pl.ds(0, tall)]
        return copy(block, block, line_send.at[k, i], line_recv.at[k, e], far)

    def start_line(k, value):
        tall = value.shape[0]
        lines[k, kind, :tall] = value
        for i in range(7):
            line_copy(k, tall, i).start()

    def relay(k, tall):
        @pl.when(c == 1)
        def _():
            def end(e, carry):
                plane_copy(k, tall, e).wait_recv()
                return carry

            lax.fori_loop(1, 16, end, 0)
            sums = jnp.sum(plane[k, :, :tall], axis=0)
            if k == 1:
                start_line(k, sums[:8])
                counts[...] = sums[8:]
            else:
                start_line(k, sums)

    def end_line(k, tall):
        for e in range(3):
            line_copy(k, tall, 2 * e).wait_recv()

        @pl.when(c == 0)
        def _():
            line_copy(k, tall, 6).wait_recv()

        return jnp.sum(lines[k, :, :tall], axis=0)

    def block_of(j):
        return full[j]

    def lanes_of(j):
        return pl.ds(pl.multiple_of(j * 256, 256), 256)

    def costs_of(j):
        return rows[j, :, :64].astype(F32).reshape(128, 256)

    def opened(j):
        return jnp.dot(plain[...], block_of(j), preferred_element_type=F32)

    def applied(k):
        def step(j, carry):
            place_columns(k, j, opened(j) * expand[j])
            return carry

        lax.fori_loop(0, 8, step, 0, unroll=2)

    def advance(k, v, ex=None):
        vectors[4] = v
        for j in range(8):
            rhs[:128, j * 256 : (j + 1) * 256] = (usage[j] + vectors[4, j : j + 1] - costs_of(j)).astype(BF16)
        if ex is not None:
            high, mid, low = three_parts(v)
            for j in range(8):
                stack = jnp.where(line == 0, high[j : j + 1], jnp.where(line == 1, mid[j : j + 1], low[j : j + 1]))
                rhs[128:, j * 256 : (j + 1) * 256] = jnp.where(line < 3, stack, 0.0).astype(BF16)

        def step(j, change):
            if ex is None:
                fresh = jnp.dot(rhs[:128], block_of(j), preferred_element_type=F32)
            else:
                both = jnp.dot(rhs[...], block_of(j), preferred_element_type=F32)
                vectors[4, pl.ds(j, 1)] = both[128:129] + both[129:130] + both[130:131]
                fresh = both[:128]
            fresh = fresh * expand[j]
            gap = fresh - usage[j]
            usage[j] = fresh
            if ex is None:
                place_columns(4, j, fresh)
            else:
                plain[:, lanes_of(j)] = (fresh - costs_of(j)).astype(BF16)
            return change + jnp.sum(gap * gap, axis=0, keepdims=True)

        plane[4, place, 7 + k : 8 + k] = lax.fori_loop(0, 8, step, jnp.zeros((1, 256), F32), unroll=2)
        if ex is not None:
            @pl.when(c == 1)
            def _():
                start_line(ex, counts[...] * vectors[4])

    def settle(total, prices, norms, k):
        mean = total * (1.0 / AGENTS)
        shared = (vectors[0] * vectors[1] + (prices + mean)) / (vectors[0] + 1.0)
        prices = prices + mean - shared
        gap = mean - shared
        norms = jnp.where(norm_lane == k - 1, float(AGENTS) * jnp.sum(gap * gap), norms)
        return shared - mean - prices, shared, prices, norms

    for j in range(8):
        rhs[:128, j * 256 : (j + 1) * 256] = -rows[j, :, :64].reshape(128, 256)

    def opening(j, change):
        fresh = jnp.dot(rhs[:128], block_of(j), preferred_element_type=F32) * expand[j]
        usage[j] = fresh
        plain[:, lanes_of(j)] = (fresh - costs_of(j)).astype(BF16)
        place_columns(0, j, fresh)
        return change + jnp.sum(fresh * fresh, axis=0, keepdims=True)

    plane[4, place, 8:9] = lax.fori_loop(0, 8, opening, jnp.zeros((1, 256), F32), unroll=2)
    start_plane(0, 8)
    for j in range(8):
        plane[1, place, 8 + j : 9 + j] = jnp.sum(expand[j], axis=0, keepdims=True)
    applied(1)
    start_plane(1, 16)
    relay(0, 8)
    relay(1, 16)
    norms = jnp.zeros((1, 128), F32)
    v, shared, prices, norms = settle(end_line(0, 8), jnp.zeros((8, 256), F32), norms, 1)
    advance(2, v, ex=5)
    applied(2)
    start_plane(2, 8)
    v, shared, prices, norms = settle(end_line(1, 8) + end_line(5, 8), prices, norms, 2)
    advance(3, v, ex=6)
    applied(3)
    start_plane(3, 8)
    relay(2, 8)
    v, shared, prices, norms = settle(end_line(2, 8) + end_line(6, 8), prices, norms, 3)
    advance(4, v, ex=7)
    relay(3, 8)
    v, shared, prices, norms = settle(end_line(3, 8) + end_line(7, 8), prices, norms, 4)
    advance(5, v)
    for e in (1, 7, 2):
        back_copy(e).start()
    plane[4, place, 13:] = jnp.zeros((3, 256), F32)
    start_plane(4, 16)
    back[kind] = usage[z, pl.ds(pl.multiple_of(c * 64, 64), 64)]
    relay(4, 16)
    for e in (1, 7, 2):
        back_copy(e).wait_recv()
    result = jnp.zeros((256, 256), F32)
    for piece in three_parts(back[...].reshape(256, 256)):
        result += lax.dot_general(
            order[...], piece.astype(BF16), (((0,), (0,)), ((), ())), preferred_element_type=F32
        )
    usage_out[...] = result
    total = end_line(4, 16)
    v, shared, prices, norms = settle(total[:8], prices, norms, 5)
    duals = jnp.zeros((1, 128), F32)
    for k in range(ITERS):
        duals = jnp.where(norm_lane == k, jnp.sum(total[8 + k : 9 + k]), duals)
    vectors[2] = shared
    vectors[3] = prices
    small_out[0:1] = vectors[2, pl.ds(z, 1)]
    small_out[1:2] = vectors[3, pl.ds(z, 1)]
    small_out[2:3, :128] = jnp.sqrt(norms + EPS)
    small_out[3:4, :128] = jnp.sqrt(duals + EPS)

    @pl.when(c == 1)
    def _():
        def end_sends(e, carry):
            for k, tall in enumerate((8, 16, 8, 8, 16)):
                plane_copy(k, tall, e).wait_send()
            return carry

        lax.fori_loop(1, 16, end_sends, 0)
        for k, tall in enumerate((8, 8, 8, 8, 16, 8, 8, 8)):
            for i in range(7):
                line_copy(k, tall, i).wait_send()

    for d in range(8):
        hand_copy(d).wait_send()
    for d in range(1, 8):
        row_copy(d).wait_send()
        z_copy(d).wait_send()
        for s in (1, 2, 3):
            one_copy(d, s).wait_send()
            two_copy(d, s).wait_send()
        core_copy(d).wait_send()
    for e in (1, 7, 2):
        back_copy(e).wait_send()


def on_device(linear_cost, agent_type, block_mask, inverses, cost_weight, target):
    vmem = pl.BlockSpec(memory_space=pltpu.VMEM)
    dma = pltpu.SemaphoreType.DMA
    usage, small = pl.pallas_call(
        kernel,
        out_shape=(jax.ShapeDtypeStruct((256, 256), F32), jax.ShapeDtypeStruct((4, 256), F32)),
        in_specs=[vmem] * 5 + [pl.BlockSpec(memory_space=pl.ANY)],
        out_specs=(vmem,) * 2,
        scratch_shapes=[
            pltpu.VMEM((4, 16, 640), BF16),
            pltpu.VMEM((2, 8, 4, 4, 16, 640), BF16),
            pltpu.VMEM((8, 2048, 256), BF16),
            pltpu.VMEM((256, 256), BF16),
            pltpu.VMEM((4, 80, 256), BF16),
            pltpu.VMEM((8, 2, 80, 256), BF16),
            pltpu.VMEM((8, 128, 256), F32),
            pltpu.VMEM((8, 128, 256), F32),
            pltpu.VMEM((144, 2048), BF16),
            pltpu.VMEM((128, 2048), BF16),
            pltpu.VMEM((8, 256), F32),
            pltpu.VMEM((5, 8, 256), F32),
            pltpu.VMEM((ITERS, 16, 16, 256), F32),
            pltpu.VMEM((8, 4, 16, 256), F32),
            pltpu.VMEM((4, 64, 256), F32),
            dma((20,)), dma((10,)),
            dma((8,)), dma((8,)),
            dma((8, 4)), dma((8, 4)),
            dma((8, 4)), dma((8, 4)),
            dma((8,)), dma((8,)),
            dma((8,)), dma((8,)),
            dma((8,)), dma((8,)),
            dma((ITERS, 16)), dma((ITERS, 16)),
            dma((8, 7)), dma((8, 4)),
            dma((8,)), dma((8,)),
        ],
        compiler_params=pltpu.CompilerParams(
            collective_id=0, has_side_effects=True, vmem_limit_bytes=60 * 2**20
        ),
        name="admm",
    )(
        linear_cost,
        agent_type.reshape(1, -1),
        block_mask.T,
        cost_weight.reshape(1, -1),
        target.reshape(1, -1),
        inverses.reshape(4, 4, 4, 16, 2048),
    )
    return usage, small[0], small[1], small[2, :ITERS], small[3, :ITERS]


def solution(mesh):
    placed = (
        P("agent", "res"),
        P("agent"),
        P("agent", "res"),
        P(None, "res", None),
        P("res"),
        P("res"),
    )
    return jax.shard_map(
        on_device,
        mesh=mesh,
        in_specs=placed,
        out_specs=(P("agent", "res"), P("res"), P("res"), P(), P()),
        check_vma=False,
    )
```

```python
import functools

import jax
import jax.numpy as jnp
from jax import lax
from jax.experimental import pallas as pl
from jax.experimental.pallas import tpu as pltpu
from jax.sharding import PartitionSpec as P

ITERS = 5
LAG_TWO, LAG_THREE, LAG_FOUR = 3, 6, 7
LAST_STEP = LAG_FOUR + 7
AGENTS = 8192
EPS = 1e-06
MESH = pl.DeviceIdType.MESH
F32 = jnp.float32
BF16 = jnp.bfloat16


def three_parts(value):
    high = value.astype(BF16).astype(F32)
    rest = value - high
    mid = rest.astype(BF16).astype(F32)
    return high, mid, rest - mid


def kernel(
    cost_hbm, type_hbm, mask_hbm, weight_hbm, target_hbm, inv_ref,
    usage_hbm, small_out,
    cost_ref, type_ref, mask_ref, weight_ref, target_ref, usage_out, stage, half, full, order, packed, rows, expand, usage, rhs, plain, counts, vectors, plane, lines, back,
    in_load, out_store, stage_load, mat_load, z_send, z_recv, one_send, one_recv, two_send, two_recv, core_send, core_recv,
    row_send, row_recv, hand_send, hand_recv, plane_send, plane_recv, line_send, line_recv, back_send, back_recv,
):
    agent, z = lax.axis_index("agent"), lax.axis_index("res")
    x, y, c = agent // 8, (agent // 2) % 4, agent % 2
    kind = z % 4
    first, second = x * (1 - c) + y * c, y * (1 - c) + x * c
    place = x * 4 + y

    def at(px, py, pc, pz):
        return (px * 8 + py * 2 + pc, pz)

    def along(step_one, step_two):
        one, two = (first + step_one) % 4, (second + step_two) % 4
        return at(one * (1 - c) + two * c, two * (1 - c) + one * c, c, z)

    def copy(src, dst, send, recv, device):
        return pltpu.make_async_remote_copy(src, dst, send, recv, device_id=device, device_id_type=MESH)

    def plane_peer(e):
        other = (place + e) % 16
        return at(other // 4, other % 4, c, z)

    barrier = pltpu.get_barrier_semaphore()

    def greet(e, carry):
        pl.semaphore_signal(barrier, inc=1, device_id=plane_peer(e), device_id_type=MESH)
        return carry

    lax.fori_loop(1, 16, greet, 0)
    for d in range(1, 8):
        pl.semaphore_signal(barrier, inc=1, device_id=at(x, y, c, (z + d) % 8), device_id_type=MESH)
    for d in (0, 1, 7, 2, 6):
        pl.semaphore_signal(barrier, inc=1, device_id=at(x, y, 1 - c, (z + d) % 8), device_id_type=MESH)
    def column(k):
        return pl.ds(pl.multiple_of(((2 * z + k) % 16) * 128, 128), 128)

    in_loads = [
        pltpu.make_async_copy(src, dst, in_load.at[i])
        for i, (src, dst) in enumerate(
            (
                (cost_hbm, cost_ref), (type_hbm, type_ref), (mask_hbm, mask_ref),
                (weight_hbm, weight_ref), (target_hbm, target_ref),
            )
        )
    ]
    for load in in_loads:
        load.start()
    own_loads = [
        pltpu.make_async_copy(
            inv_ref.at[t, first, second, :, column(c * 5 + i)],
            stage.at[t, :, pl.ds(i * 128, 128)],
            stage_load.at[t * 5 + i],
        )
        for t in range(4)
        for i in range(5)
    ] + [
        pltpu.make_async_copy(
            inv_ref.at[kind, :, :, :, column(k)],
            half.at[k // 5, z, :, :, :, pl.ds((k % 5) * 128, 128)],
            mat_load.at[k],
        )
        for k in range(10)
    ]
    for load in own_loads:
        load.start()
    def z_copy(d):
        far = (z + d) % 8
        return copy(
            stage.at[far % 4], half.at[c, z, first, second], z_send.at[d], z_recv.at[d], at(x, y, c, far)
        )


    for load in in_loads:
        load.wait()
    kinds = type_ref[...]
    is_kind = (lax.broadcasted_iota(jnp.int32, (16, 256), 0) == kinds).astype(F32)
    before = (
        lax.broadcasted_iota(jnp.int32, (256, 256), 0) < lax.broadcasted_iota(jnp.int32, (256, 256), 1)
    ).astype(BF16)
    ahead = jnp.dot(is_kind.astype(BF16), before, preferred_element_type=F32)
    spot = kinds * 64 + jnp.sum(is_kind * ahead, axis=0, keepdims=True).astype(jnp.int32)
    order[...] = (lax.broadcasted_iota(jnp.int32, (256, 256), 0) == spot).astype(F32).astype(BF16)
    cost = jnp.dot(order[...], cost_ref[...].astype(BF16), preferred_element_type=F32).astype(BF16)
    extra = jnp.concatenate(
        [mask_ref[...].astype(F32), jnp.zeros((14, 256), F32)], axis=0
    ).astype(BF16)
    masks = lax.dot_general(extra, order[...], (((1,), (1,)), ((), ())), preferred_element_type=F32)
    line = lax.broadcasted_iota(jnp.int32, (16, 256), 0)
    lane = lax.broadcasted_iota(jnp.int32, (16, 256), 1)
    tail = jnp.zeros((16, 256), F32)
    for r, part in enumerate(three_parts(weight_ref[...]) + three_parts(target_ref[...])):
        tail = jnp.where(line == 2 + r, part, tail)
    for t in range(4):
        packed[t, :64] = cost[t * 64 : (t + 1) * 64]
        turned = masks if t == 0 else pltpu.roll(masks, 256 - 64 * t, 1)
        packed[t, 64:] = jnp.where((line < 2) & (lane < 64), turned, tail).astype(BF16)

    def row_copy(d):
        far = (z + d) % 8
        return copy(packed.at[far % 4], rows.at[z, c], row_send.at[d], row_recv.at[d], at(x, y, c, far))

    def hand_copy(d):
        block = rows.at[(z - d + 8) % 8, c]
        return copy(block, block, hand_send.at[d], hand_recv.at[d], at(x, y, 1 - c, z))

    for load in own_loads[:20]:
        load.wait()
    pl.semaphore_wait(barrier, 27)
    for d in (1, 7, 2, 6, 3, 5, 4):
        z_copy(d).start()
    for d in (1, 7, 2, 6, 3, 5, 4):
        row_copy(d).start()
    rows[z, c] = packed[kind]
    hand_copy(0).start()

    def part(d):
        return half.at[c, (z - d + 8) % 8]

    def one_copy(d, s):
        block = part(d).at[first, second]
        return copy(block, block, one_send.at[d, s], one_recv.at[d, s], along(s, 0))

    def two_copy(d, s):
        block = part(d).at[:, second]
        return copy(block, block, two_send.at[d, s], two_recv.at[d, s], along(0, s))

    def core_copy(d):
        return copy(part(d), part(d), core_send.at[d], core_recv.at[d], at(x, y, 1 - c, z))

    line = lax.broadcasted_iota(jnp.int32, (16, 256), 0)
    wide = (lax.broadcasted_iota(jnp.int32, (16, 256), 1) // 128 == line).astype(F32).astype(BF16)

    def fill(block):
        for k in range(10):
            tile = half[k // 5, block, :, :, :, (k % 5) * 128 : (k % 5) * 128 + 128].reshape(256, 128)
            across = (block + k // 2) % 8
            full[across, pl.ds(pl.multiple_of(block * 256, 256), 256), (k % 2) * 128 : (k % 2) * 128 + 128] = tile
            if 2 <= k < 8:
                full[block, pl.ds(pl.multiple_of(across * 256 + (k % 2) * 128, 128), 128), :] = tile.T

    def first_product(block):
        for j in range(5):
            across = (block + j) % 8
            usage[across] += jnp.dot(
                rows[block, :, :64].reshape(128, 256),
                full[across, pl.ds(pl.multiple_of(block * 256, 256), 256), :],
                preferred_element_type=F32,
            )
        mirror = jnp.zeros((128, 256), F32)
        for j in range(1, 4):
            across = (block + j) % 8
            mirror += jnp.dot(
                rows[across, :, :64].reshape(128, 256),
                full[block, pl.ds(pl.multiple_of(across * 256, 256), 256), :],
                preferred_element_type=F32,
            )
        usage[block] += mirror

    def stage_one(d):
        z_copy(d).wait_recv()
        for s in (2, 1, 3):
            one_copy(d, s).start()

    def stage_two(d):
        for s in (2, 1, 3):
            one_copy(d, s).wait_recv()
        for s in (2, 1, 3):
            two_copy(d, s).start()

    def stage_three(d):
        for s in (2, 1, 3):
            two_copy(d, s).wait_recv()
        core_copy(d).start()

    def stage_four(d):
        core_copy(d).wait_recv()
        fill((z - d + 8) % 8)
        first_product((z - d + 8) % 8)

    def unpack():
        for d in (1, 7, 2, 6, 3, 5, 4):
            row_copy(d).wait_recv()
            hand_copy(d).start()
        for load in own_loads[20:]:
            load.wait()
        fill(z)
        for d in range(8):
            hand_copy(d).wait_recv()
        for j in range(8):
            ends = rows[j, 0, 64:].astype(F32)
            vectors[0, j : j + 1] = ends[2:3] + ends[3:4] + ends[4:5]
            vectors[1, j : j + 1] = ends[5:6] + ends[6:7] + ends[7:8]
            for side in range(2):
                here = rows[j, side, 64:, :128]
                spread = lax.dot_general(here, wide, (((0,), (0,)), ((), ())), preferred_element_type=F32)
                expand[j, side * 64 : side * 64 + 64] = spread[:64]
        usage[...] = jnp.zeros((8, 128, 256), F32)
        first_product(z)

    turns = (1, 7, 2, 6, 3, 5, 4)
    for step in range(LAST_STEP):
        for lag, act in ((0, stage_one), (LAG_TWO, stage_two), (LAG_THREE, stage_three), (LAG_FOUR, stage_four)):
            if 0 <= step - lag < 7:
                act(turns[step - lag])
        if step == LAG_FOUR - 1:
            unpack()

    norm_lane = lax.broadcasted_iota(jnp.int32, (1, 128), 1)

    def back_copy(e):
        far = (z + e) % 8
        return copy(
            usage.at[far, pl.ds(pl.multiple_of(c * 64, 64), 64)],
            back.at[kind],
            back_send.at[e],
            back_recv.at[e],
            at(x, y, c, far),
        )

    def place_columns(k, j, value):
        plane[k, place, pl.ds(j, 1)] = jnp.sum(value, axis=0, keepdims=True)

    def plane_copy(k, tall, e):
        block = plane.at[k, place, pl.ds(0, tall)]
        return copy(block, block, plane_send.at[k, e], plane_recv.at[k, e], plane_peer(e))

    def start_plane(k, tall):
        @pl.when(c == 1)
        def _():
            def start(e, carry):
                plane_copy(k, tall, e).start()
                return carry

            lax.fori_loop(1, 16, start, 0)

    def line_copy(k, tall, i):
        e = i // 2
        far = at(x, y, 1 - c, z) if e == 3 else at(x, y, 1 - i % 2, (z + (1, 7, 2)[e]) % 8)
        block = lines.at[k, kind, pl.ds(0, tall)]
        return copy(block, block, line_send.at[k, i], line_recv.at[k, e], far)

    def start_line(k, value):
        tall = value.shape[0]
        lines[k, kind, :tall] = value
        for i in range(7):
            line_copy(k, tall, i).start()

    def relay(k, tall):
        @pl.when(c == 1)
        def _():
            def end(e, carry):
                plane_copy(k, tall, e).wait_recv()
                return carry

            lax.fori_loop(1, 16, end, 0)
            sums = jnp.sum(plane[k, :, :tall], axis=0)
            if k == 1:
                start_line(k, sums[:8])
                counts[...] = sums[8:]
            else:
                start_line(k, sums)

    def end_line(k, tall):
        for e in range(3):
            line_copy(k, tall, 2 * e).wait_recv()

        @pl.when(c == 0)
        def _():
            line_copy(k, tall, 6).wait_recv()

        return jnp.sum(lines[k, :, :tall], axis=0)

    def block_of(j):
        return full[j]

    def lanes_of(j):
        return pl.ds(pl.multiple_of(j * 256, 256), 256)

    def costs_of(j):
        return rows[j, :, :64].astype(F32).reshape(128, 256)

    def opened(j):
        return jnp.dot(plain[...], block_of(j), preferred_element_type=F32)

    def applied(k):
        def step(j, carry):
            place_columns(k, j, opened(j) * expand[j])
            return carry

        lax.fori_loop(0, 8, step, 0, unroll=2)

    def advance(k, v, ex=None):
        vectors[4] = v
        for j in range(8):
            rhs[:128, j * 256 : (j + 1) * 256] = (usage[j] + vectors[4, j : j + 1] - costs_of(j)).astype(BF16)
        if ex is not None:
            high, mid, low = three_parts(v)
            for j in range(8):
                stack = jnp.where(line == 0, high[j : j + 1], jnp.where(line == 1, mid[j : j + 1], low[j : j + 1]))
                rhs[128:, j * 256 : (j + 1) * 256] = jnp.where(line < 3, stack, 0.0).astype(BF16)

        def step(j, change):
            if ex is None:
                fresh = jnp.dot(rhs[:128], block_of(j), preferred_element_type=F32)
            else:
                both = jnp.dot(rhs[...], block_of(j), preferred_element_type=F32)
                vectors[4, pl.ds(j, 1)] = both[128:129] + both[129:130] + both[130:131]
                fresh = both[:128]
            fresh = fresh * expand[j]
            gap = fresh - usage[j]
            usage[j] = fresh
            if ex is None:
                place_columns(4, j, fresh)
            else:
                plain[:, lanes_of(j)] = (fresh - costs_of(j)).astype(BF16)
            return change + jnp.sum(gap * gap, axis=0, keepdims=True)

        plane[4, place, 7 + k : 8 + k] = lax.fori_loop(0, 8, step, jnp.zeros((1, 256), F32), unroll=2)
        if ex is not None:
            @pl.when(c == 1)
            def _():
                start_line(ex, counts[...] * vectors[4])

    def settle(total, prices, norms, k):
        mean = total * (1.0 / AGENTS)
        shared = (vectors[0] * vectors[1] + (prices + mean)) / (vectors[0] + 1.0)
        prices = prices + mean - shared
        gap = mean - shared
        norms = jnp.where(norm_lane == k - 1, float(AGENTS) * jnp.sum(gap * gap), norms)
        return shared - mean - prices, shared, prices, norms

    def opening(j, change):
        fresh = -usage[j] * expand[j]
        usage[j] = fresh
        plain[:, lanes_of(j)] = (fresh - costs_of(j)).astype(BF16)
        place_columns(0, j, fresh)
        return change + jnp.sum(fresh * fresh, axis=0, keepdims=True)

    plane[4, place, 8:9] = lax.fori_loop(0, 8, opening, jnp.zeros((1, 256), F32), unroll=2)
    start_plane(0, 8)
    for j in range(8):
        plane[1, place, 8 + j : 9 + j] = jnp.sum(expand[j], axis=0, keepdims=True)
    applied(1)
    start_plane(1, 16)
    relay(0, 8)
    relay(1, 16)
    norms = jnp.zeros((1, 128), F32)
    v, shared, prices, norms = settle(end_line(0, 8), jnp.zeros((8, 256), F32), norms, 1)
    advance(2, v, ex=5)
    applied(2)
    start_plane(2, 8)
    v, shared, prices, norms = settle(end_line(1, 8) + end_line(5, 8), prices, norms, 2)
    advance(3, v, ex=6)
    applied(3)
    start_plane(3, 8)
    relay(2, 8)
    v, shared, prices, norms = settle(end_line(2, 8) + end_line(6, 8), prices, norms, 3)
    advance(4, v, ex=7)
    relay(3, 8)
    v, shared, prices, norms = settle(end_line(3, 8) + end_line(7, 8), prices, norms, 4)
    advance(5, v)
    for e in (1, 7, 2):
        back_copy(e).start()
    plane[4, place, 13:] = jnp.zeros((3, 256), F32)
    start_plane(4, 16)
    back[kind] = usage[z, pl.ds(pl.multiple_of(c * 64, 64), 64)]
    relay(4, 16)
    for e in (1, 7, 2):
        back_copy(e).wait_recv()
    result = jnp.zeros((256, 256), F32)
    for piece in three_parts(back[...].reshape(256, 256)):
        result += lax.dot_general(
            order[...], piece.astype(BF16), (((0,), (0,)), ((), ())), preferred_element_type=F32
        )
    usage_out[...] = result
    usage_store = pltpu.make_async_copy(usage_out, usage_hbm, out_store)
    usage_store.start()
    total = end_line(4, 16)
    v, shared, prices, norms = settle(total[:8], prices, norms, 5)
    duals = jnp.zeros((1, 128), F32)
    for k in range(ITERS):
        duals = jnp.where(norm_lane == k, jnp.sum(total[8 + k : 9 + k]), duals)
    vectors[2] = shared
    vectors[3] = prices
    small_out[0:1] = vectors[2, pl.ds(z, 1)]
    small_out[1:2] = vectors[3, pl.ds(z, 1)]
    small_out[2:3, :128] = jnp.sqrt(norms + EPS)
    small_out[3:4, :128] = jnp.sqrt(duals + EPS)
    usage_store.wait()

    @pl.when(c == 1)
    def _():
        def end_sends(e, carry):
            for k, tall in enumerate((8, 16, 8, 8, 16)):
                plane_copy(k, tall, e).wait_send()
            return carry

        lax.fori_loop(1, 16, end_sends, 0)
        for k, tall in enumerate((8, 8, 8, 8, 16, 8, 8, 8)):
            for i in range(7):
                line_copy(k, tall, i).wait_send()

    for d in range(8):
        hand_copy(d).wait_send()
    for d in range(1, 8):
        row_copy(d).wait_send()
        z_copy(d).wait_send()
        for s in (1, 2, 3):
            one_copy(d, s).wait_send()
            two_copy(d, s).wait_send()
        core_copy(d).wait_send()
    for e in (1, 7, 2):
        back_copy(e).wait_send()


def hand_over(usage_ref, small_ref, usage_out, shared_out, prices_out, primal_out, dual_out):
    usage_out[...] = usage_ref[...]
    shared_out[...] = small_ref[0:1]
    prices_out[...] = small_ref[1:2]
    primal_out[...] = small_ref[2:3, :ITERS]
    dual_out[...] = small_ref[3:4, :ITERS]


def on_device(linear_cost, agent_type, block_mask, inverses, cost_weight, target):
    vmem = pl.BlockSpec(memory_space=pltpu.VMEM)
    anywhere = pl.BlockSpec(memory_space=pl.ANY)
    dma = pltpu.SemaphoreType.DMA
    usage, small = pl.pallas_call(
        kernel,
        out_shape=(jax.ShapeDtypeStruct((256, 256), F32), jax.ShapeDtypeStruct((4, 256), F32)),
        in_specs=[anywhere] * 6,
        out_specs=(anywhere, vmem),
        scratch_shapes=[
            pltpu.VMEM((256, 256), F32),
            pltpu.VMEM((1, 256), jnp.int32),
            pltpu.VMEM((2, 256), jnp.int32),
            pltpu.VMEM((1, 256), F32),
            pltpu.VMEM((1, 256), F32),
            pltpu.VMEM((256, 256), F32),
            pltpu.VMEM((4, 16, 640), BF16),
            pltpu.VMEM((2, 8, 4, 4, 16, 640), BF16),
            pltpu.VMEM((8, 2048, 256), BF16),
            pltpu.VMEM((256, 256), BF16),
            pltpu.VMEM((4, 80, 256), BF16),
            pltpu.VMEM((8, 2, 80, 256), BF16),
            pltpu.VMEM((8, 128, 256), F32),
            pltpu.VMEM((8, 128, 256), F32),
            pltpu.VMEM((144, 2048), BF16),
            pltpu.VMEM((128, 2048), BF16),
            pltpu.VMEM((8, 256), F32),
            pltpu.VMEM((5, 8, 256), F32),
            pltpu.VMEM((ITERS, 16, 16, 256), F32),
            pltpu.VMEM((8, 4, 16, 256), F32),
            pltpu.VMEM((4, 64, 256), F32),
            dma((5,)), dma, dma((20,)), dma((10,)),
            dma((8,)), dma((8,)),
            dma((8, 4)), dma((8, 4)),
            dma((8, 4)), dma((8, 4)),
            dma((8,)), dma((8,)),
            dma((8,)), dma((8,)),
            dma((8,)), dma((8,)),
            dma((ITERS, 16)), dma((ITERS, 16)),
            dma((8, 7)), dma((8, 4)),
            dma((8,)), dma((8,)),
        ],
        compiler_params=pltpu.CompilerParams(
            collective_id=0, has_side_effects=True, vmem_limit_bytes=60 * 2**20
        ),
        name="admm",
    )(
        linear_cost,
        agent_type.reshape(1, -1),
        block_mask.T,
        cost_weight.reshape(1, -1),
        target.reshape(1, -1),
        inverses.reshape(4, 4, 4, 16, 2048),
    )
    usage, shared, prices, primal, dual = pl.pallas_call(
        hand_over,
        out_shape=(
            jax.ShapeDtypeStruct((256, 256), F32),
            jax.ShapeDtypeStruct((1, 256), F32),
            jax.ShapeDtypeStruct((1, 256), F32),
            jax.ShapeDtypeStruct((1, ITERS), F32),
            jax.ShapeDtypeStruct((1, ITERS), F32),
        ),
        in_specs=[vmem] * 2,
        out_specs=(vmem,) * 5,
        name="hand_over",
    )(usage, small)
    return usage, shared.reshape(-1), prices.reshape(-1), primal.reshape(-1), dual.reshape(-1)


def solution(mesh):
    placed = (
        P("agent", "res"),
        P("agent"),
        P("agent", "res"),
        P(None, "res", None),
        P("res"),
        P("res"),
    )
    return jax.shard_map(
        on_device,
        mesh=mesh,
        in_specs=placed,
        out_specs=(P("agent", "res"), P("res"), P("res"), P(), P()),
        check_vma=False,
    )
```

```python
import functools

import jax
import jax.numpy as jnp
from jax import lax
from jax.experimental import pallas as pl
from jax.experimental.pallas import tpu as pltpu
from jax.sharding import PartitionSpec as P

ITERS = 5
LAG_TWO, LAG_THREE, LAG_FOUR = 3, 6, 7
LAST_STEP = LAG_FOUR + 7
AGENTS = 8192
EPS = 1e-06
MESH = pl.DeviceIdType.MESH
F32 = jnp.float32
BF16 = jnp.bfloat16


def three_parts(value):
    high = value.astype(BF16).astype(F32)
    rest = value - high
    mid = rest.astype(BF16).astype(F32)
    return high, mid, rest - mid


def kernel(
    cost_hbm, type_hbm, mask_hbm, weight_hbm, target_hbm, inv_ref,
    usage_hbm, small_out,
    cost_ref, type_ref, mask_ref, weight_ref, target_ref, usage_out, stage, half, full, order, packed, rows, expand, usage, rhs, plain, counts, vectors, plane, lines, back,
    in_load, out_store, stage_load, mat_load, z_send, z_recv, one_send, one_recv, two_send, two_recv, core_send, core_recv,
    row_send, row_recv, hand_send, hand_recv, plane_send, plane_recv, line_send, line_recv, back_send, back_recv,
):
    agent, z = lax.axis_index("agent"), lax.axis_index("res")
    x, y, c = agent // 8, (agent // 2) % 4, agent % 2
    kind = z % 4
    first, second = x * (1 - c) + y * c, y * (1 - c) + x * c
    place = x * 4 + y

    def at(px, py, pc, pz):
        return (px * 8 + py * 2 + pc, pz)

    def along(step_one, step_two):
        one, two = (first + step_one) % 4, (second + step_two) % 4
        return at(one * (1 - c) + two * c, two * (1 - c) + one * c, c, z)

    def copy(src, dst, send, recv, device):
        return pltpu.make_async_remote_copy(src, dst, send, recv, device_id=device, device_id_type=MESH)

    def plane_peer(e):
        other = (place + e) % 16
        return at(other // 4, other % 4, c, z)

    barrier = pltpu.get_barrier_semaphore()

    def greet(e, carry):
        pl.semaphore_signal(barrier, inc=1, device_id=plane_peer(e), device_id_type=MESH)
        return carry

    lax.fori_loop(1, 16, greet, 0)
    for d in range(1, 8):
        pl.semaphore_signal(barrier, inc=1, device_id=at(x, y, c, (z + d) % 8), device_id_type=MESH)
    for d in (0, 1, 7, 2, 6):
        pl.semaphore_signal(barrier, inc=1, device_id=at(x, y, 1 - c, (z + d) % 8), device_id_type=MESH)
    def column(k):
        return pl.ds(pl.multiple_of(((2 * z + k) % 16) * 128, 128), 128)

    in_loads = [
        pltpu.make_async_copy(src, dst, in_load.at[i])
        for i, (src, dst) in enumerate(
            (
                (cost_hbm, cost_ref), (type_hbm, type_ref), (mask_hbm, mask_ref),
                (weight_hbm, weight_ref), (target_hbm, target_ref),
            )
        )
    ]
    for load in in_loads:
        load.start()
    own_loads = [
        pltpu.make_async_copy(
            inv_ref.at[t, first, second, :, column(c * 4 + i + (i // 4) * (4 - 3 * c))],
            stage.at[t, :, pl.ds(i * 128, 128)],
            stage_load.at[t * 5 + i],
        )
        for t in range(4)
        for i in range(5)
    ] + [
        pltpu.make_async_copy(
            inv_ref.at[kind, :, :, :, column(k)],
            half.at[(k // 4 if k < 8 else k - 8), z, :, :, :, pl.ds((k % 4 if k < 8 else 4) * 128, 128)],
            mat_load.at[k],
        )
        for k in range(10)
    ]
    for load in own_loads:
        load.start()
    def sized(source, act):
        @pl.when(source < 4)
        def _():
            act(640)

        @pl.when(source >= 4)
        def _():
            act(512)

    def z_copy(d, width):
        far = (z + d) % 8
        return copy(
            stage.at[far % 4, :, :width],
            half.at[c, z, first, second, :, :width],
            z_send.at[d],
            z_recv.at[d],
            at(x, y, c, far),
        )

    for load in own_loads[:20]:
        load.wait()
    pl.semaphore_wait(barrier, 27)

    def start_parts(width):
        for d in (1, 7, 2, 6, 3, 5, 4):
            z_copy(d, width).start()

    sized(z, start_parts)

    for load in in_loads:
        load.wait()
    kinds = type_ref[...]
    is_kind = (lax.broadcasted_iota(jnp.int32, (16, 256), 0) == kinds).astype(F32)
    before = (
        lax.broadcasted_iota(jnp.int32, (256, 256), 0) < lax.broadcasted_iota(jnp.int32, (256, 256), 1)
    ).astype(BF16)
    ahead = jnp.dot(is_kind.astype(BF16), before, preferred_element_type=F32)
    spot = kinds * 64 + jnp.sum(is_kind * ahead, axis=0, keepdims=True).astype(jnp.int32)
    order[...] = (lax.broadcasted_iota(jnp.int32, (256, 256), 0) == spot).astype(F32).astype(BF16)
    cost = jnp.dot(order[...], cost_ref[...].astype(BF16), preferred_element_type=F32).astype(BF16)
    extra = jnp.concatenate(
        [mask_ref[...].astype(F32), jnp.zeros((14, 256), F32)], axis=0
    ).astype(BF16)
    masks = lax.dot_general(extra, order[...], (((1,), (1,)), ((), ())), preferred_element_type=F32)
    line = lax.broadcasted_iota(jnp.int32, (16, 256), 0)
    lane = lax.broadcasted_iota(jnp.int32, (16, 256), 1)
    tail = jnp.zeros((16, 256), F32)
    for r, part in enumerate(three_parts(weight_ref[...]) + three_parts(target_ref[...])):
        tail = jnp.where(line == 2 + r, part, tail)
    for t in range(4):
        packed[t, :64] = cost[t * 64 : (t + 1) * 64]
        turned = masks if t == 0 else pltpu.roll(masks, 256 - 64 * t, 1)
        packed[t, 64:] = jnp.where((line < 2) & (lane < 64), turned, tail).astype(BF16)

    def row_copy(d):
        far = (z + d) % 8
        return copy(packed.at[far % 4], rows.at[z, c], row_send.at[d], row_recv.at[d], at(x, y, c, far))

    def hand_copy(d):
        block = rows.at[(z - d + 8) % 8, c]
        return copy(block, block, hand_send.at[d], hand_recv.at[d], at(x, y, 1 - c, z))

    for d in (1, 7, 2, 6, 3, 5, 4):
        row_copy(d).start()
    rows[z, c] = packed[kind]
    hand_copy(0).start()

    def source(d):
        return (z - d + 8) % 8

    def one_copy(d, s, width):
        block = half.at[c, source(d), first, second, :, :width]
        return copy(block, block, one_send.at[d, s], one_recv.at[d, s], along(s, 0))

    def two_copy(d, s, width):
        block = half.at[c, source(d), :, second, :, :width]
        return copy(block, block, two_send.at[d, s], two_recv.at[d, s], along(0, s))

    def core_copy(d, width):
        block = half.at[c, source(d), :, :, :, :width]
        return copy(block, block, core_send.at[d], core_recv.at[d], at(x, y, 1 - c, z))

    line = lax.broadcasted_iota(jnp.int32, (16, 256), 0)
    wide = (lax.broadcasted_iota(jnp.int32, (16, 256), 1) // 128 == line).astype(F32).astype(BF16)

    def fill_tiles(block, picked):
        for k in picked:
            side, spot_ = (k // 4, k % 4) if k < 8 else (k - 8, 4)
            tile = half[side, block, :, :, :, spot_ * 128 : spot_ * 128 + 128].reshape(256, 128)
            across = (block + k // 2) % 8
            full[across, pl.ds(pl.multiple_of(block * 256, 256), 256), (k % 2) * 128 : (k % 2) * 128 + 128] = tile
            if k >= 2:
                full[block, pl.ds(pl.multiple_of(across * 256 + (k % 2) * 128, 128), 128), :] = tile.T

    def times(row_block, column_block):
        return jnp.dot(
            rows[row_block, :, :64].reshape(128, 256),
            full[column_block, pl.ds(pl.multiple_of(row_block * 256, 256), 256), :],
            preferred_element_type=F32,
        )

    def fill(block):
        fill_tiles(block, range(8))
        for j in range(4):
            across = (block + j) % 8
            usage[across] += times(block, across)
        mirror = jnp.zeros((128, 256), F32)
        for j in range(1, 4):
            mirror += times((block + j) % 8, block)
        usage[block] += mirror

        @pl.when(block < 4)
        def _():
            across = (block + 4) % 8
            fill_tiles(block, (8, 9))
            usage[across] += times(block, across)
            usage[block] += times(across, block)

    def stage_one(d, width):
        z_copy(d, width).wait_recv()
        for s in (2, 1, 3):
            one_copy(d, s, width).start()

    def stage_two(d, width):
        for s in (2, 1, 3):
            one_copy(d, s, width).wait_recv()
        for s in (2, 1, 3):
            two_copy(d, s, width).start()

    def stage_three(d, width):
        for s in (2, 1, 3):
            two_copy(d, s, width).wait_recv()
        core_copy(d, width).start()

    def stage_four(d, width):
        core_copy(d, width).wait_recv()

    def end_parts(d, width):
        for s in (1, 2, 3):
            one_copy(d, s, width).wait_send()
            two_copy(d, s, width).wait_send()
        core_copy(d, width).wait_send()

    def unpack():
        for d in (1, 7, 2, 6, 3, 5, 4):
            row_copy(d).wait_recv()
            hand_copy(d).start()
        for load in own_loads[20:]:
            load.wait()
        for d in range(8):
            hand_copy(d).wait_recv()
        for j in range(8):
            ends = rows[j, 0, 64:].astype(F32)
            vectors[0, j : j + 1] = ends[2:3] + ends[3:4] + ends[4:5]
            vectors[1, j : j + 1] = ends[5:6] + ends[6:7] + ends[7:8]
            for side in range(2):
                here = rows[j, side, 64:, :128]
                spread = lax.dot_general(here, wide, (((0,), (0,)), ((), ())), preferred_element_type=F32)
                expand[j, side * 64 : side * 64 + 64] = spread[:64]
        usage[...] = jnp.zeros((8, 128, 256), F32)
        fill(z)

    turns = (1, 7, 2, 6, 3, 5, 4)
    for step in range(LAST_STEP):
        for lag, act in ((0, stage_one), (LAG_TWO, stage_two), (LAG_THREE, stage_three), (LAG_FOUR, stage_four)):
            if 0 <= step - lag < 7:
                sized(source(turns[step - lag]), functools.partial(act, turns[step - lag]))
                if act is stage_four:
                    fill(source(turns[step - lag]))
        if step == LAG_FOUR - 1:
            unpack()

    norm_lane = lax.broadcasted_iota(jnp.int32, (1, 128), 1)

    def back_copy(e):
        far = (z + e) % 8
        return copy(
            usage.at[far, pl.ds(pl.multiple_of(c * 64, 64), 64)],
            back.at[kind],
            back_send.at[e],
            back_recv.at[e],
            at(x, y, c, far),
        )

    def place_columns(k, j, value):
        plane[k, place, pl.ds(j, 1)] = jnp.sum(value, axis=0, keepdims=True)

    def plane_copy(k, tall, e):
        block = plane.at[k, place, pl.ds(0, tall)]
        return copy(block, block, plane_send.at[k, e], plane_recv.at[k, e], plane_peer(e))

    def start_plane(k, tall):
        @pl.when(c == 1)
        def _():
            def start(e, carry):
                plane_copy(k, tall, e).start()
                return carry

            lax.fori_loop(1, 16, start, 0)

    def line_copy(k, tall, i):
        e = i // 2
        far = at(x, y, 1 - c, z) if e == 3 else at(x, y, 1 - i % 2, (z + (1, 7, 2)[e]) % 8)
        block = lines.at[k, kind, pl.ds(0, tall)]
        return copy(block, block, line_send.at[k, i], line_recv.at[k, e], far)

    def start_line(k, value):
        tall = value.shape[0]
        lines[k, kind, :tall] = value
        for i in range(7):
            line_copy(k, tall, i).start()

    def relay(k, tall):
        @pl.when(c == 1)
        def _():
            def end(e, carry):
                plane_copy(k, tall, e).wait_recv()
                return carry

            lax.fori_loop(1, 16, end, 0)
            sums = jnp.sum(plane[k, :, :tall], axis=0)
            if k == 1:
                start_line(k, sums[:8])
                counts[...] = sums[8:]
            else:
                start_line(k, sums)

    def end_line(k, tall):
        for e in range(3):
            line_copy(k, tall, 2 * e).wait_recv()

        @pl.when(c == 0)
        def _():
            line_copy(k, tall, 6).wait_recv()

        return jnp.sum(lines[k, :, :tall], axis=0)

    def block_of(j):
        return full[j]

    def lanes_of(j):
        return pl.ds(pl.multiple_of(j * 256, 256), 256)

    def costs_of(j):
        return rows[j, :, :64].astype(F32).reshape(128, 256)

    def opened(j):
        return jnp.dot(plain[...], block_of(j), preferred_element_type=F32)

    def applied(k):
        def step(j, carry):
            place_columns(k, j, opened(j) * expand[j])
            return carry

        lax.fori_loop(0, 8, step, 0, unroll=2)

    def advance(k, v, ex=None):
        vectors[4] = v
        high, mid, low = three_parts(v)
        for j in range(8):
            rhs[:128, j * 256 : (j + 1) * 256] = (usage[j] + vectors[4, j : j + 1] - costs_of(j)).astype(BF16)
            stack = jnp.where(line == 0, high[j : j + 1], jnp.where(line == 1, mid[j : j + 1], low[j : j + 1]))
            rhs[128:, j * 256 : (j + 1) * 256] = jnp.where(line < 3, stack, 0.0).astype(BF16)

        def step(j, change):
            both = jnp.dot(rhs[...], block_of(j), preferred_element_type=F32)
            vectors[4, pl.ds(j, 1)] = both[128:129] + both[129:130] + both[130:131]
            fresh = both[:128] * expand[j]
            gap = fresh - usage[j]
            usage[j] = fresh
            if ex is not None:
                plain[:, lanes_of(j)] = (fresh - costs_of(j)).astype(BF16)
            return change + jnp.sum(gap * gap, axis=0, keepdims=True)

        change = lax.fori_loop(0, 8, step, jnp.zeros((1, 256), F32), unroll=2)
        if ex is not None:
            plane[4, place, 7 + k : 8 + k] = change

            @pl.when(c == 1)
            def _():
                start_line(ex, counts[...] * vectors[4])

    def foreseen():
        vectors[5] = vectors[4]

        def step(j, change):
            gap = (opened(j) + vectors[5, pl.ds(j, 1)]) * expand[j] - usage[j]
            place_columns(4, j, gap)
            return change + jnp.sum(gap * gap, axis=0, keepdims=True)

        plane[4, place, 12:13] = lax.fori_loop(0, 8, step, jnp.zeros((1, 256), F32), unroll=2)
        plane[4, place, 13:] = jnp.zeros((3, 256), F32)

    def relay_last():
        @pl.when(c == 1)
        def _():
            def end(e, carry):
                plane_copy(4, 16, e).wait_recv()
                return carry

            lax.fori_loop(1, 16, end, 0)
            sums = jnp.sum(plane[4], axis=0)
            step = vectors[4] - vectors[5]
            gaps, masks_ = sums[:8], counts[...]
            square = jnp.sum((2.0 * gaps + masks_ * step) * step, axis=0, keepdims=True)
            row = lax.broadcasted_iota(jnp.int32, (8, 256), 0)
            tail_ = sums[8:] + jnp.where(row == 4, square, 0.0)
            start_line(4, jnp.concatenate([gaps + masks_ * step, tail_], axis=0))

    def settle(total, prices, norms, k):
        mean = total * (1.0 / AGENTS)
        shared = (vectors[0] * vectors[1] + (prices + mean)) / (vectors[0] + 1.0)
        prices = prices + mean - shared
        gap = mean - shared
        norms = jnp.where(norm_lane == k - 1, float(AGENTS) * jnp.sum(gap * gap), norms)
        return shared - mean - prices, shared, prices, norms

    def opening(j, change):
        fresh = -usage[j] * expand[j]
        usage[j] = fresh
        plain[:, lanes_of(j)] = (fresh - costs_of(j)).astype(BF16)
        place_columns(0, j, fresh)
        return change + jnp.sum(fresh * fresh, axis=0, keepdims=True)

    plane[4, place, 8:9] = lax.fori_loop(0, 8, opening, jnp.zeros((1, 256), F32), unroll=2)
    start_plane(0, 8)
    for j in range(8):
        plane[1, place, 8 + j : 9 + j] = jnp.sum(expand[j], axis=0, keepdims=True)
    applied(1)
    start_plane(1, 16)
    relay(0, 8)
    relay(1, 16)
    norms = jnp.zeros((1, 128), F32)
    v, shared, prices, norms = settle(end_line(0, 8), jnp.zeros((8, 256), F32), norms, 1)
    advance(2, v, ex=5)
    applied(2)
    start_plane(2, 8)
    v, shared, prices, norms = settle(end_line(1, 8) + end_line(5, 8), prices, norms, 2)
    advance(3, v, ex=6)
    applied(3)
    start_plane(3, 8)
    relay(2, 8)
    v, shared, prices, norms = settle(end_line(2, 8) + end_line(6, 8), prices, norms, 3)
    advance(4, v, ex=7)
    relay(3, 8)
    foreseen()
    start_plane(4, 16)
    usage_sum = end_line(3, 8) + end_line(7, 8)
    v, shared, prices, norms = settle(usage_sum, prices, norms, 4)
    advance(5, v)
    for e in (1, 7, 2):
        back_copy(e).start()
    back[kind] = usage[z, pl.ds(pl.multiple_of(c * 64, 64), 64)]
    relay_last()
    for e in (1, 7, 2):
        back_copy(e).wait_recv()
    result = jnp.zeros((256, 256), F32)
    for piece in three_parts(back[...].reshape(256, 256)):
        result += lax.dot_general(
            order[...], piece.astype(BF16), (((0,), (0,)), ((), ())), preferred_element_type=F32
        )
    usage_out[...] = result
    usage_store = pltpu.make_async_copy(usage_out, usage_hbm, out_store)
    usage_store.start()
    total = end_line(4, 16)
    v, shared, prices, norms = settle(usage_sum + total[:8], prices, norms, 5)
    duals = jnp.zeros((1, 128), F32)
    for k in range(ITERS):
        duals = jnp.where(norm_lane == k, jnp.sum(total[8 + k : 9 + k]), duals)
    vectors[2] = shared
    vectors[3] = prices
    small_out[0:1] = vectors[2, pl.ds(z, 1)]
    small_out[1:2] = vectors[3, pl.ds(z, 1)]
    small_out[2:3, :128] = jnp.sqrt(norms + EPS)
    small_out[3:4, :128] = jnp.sqrt(duals + EPS)
    usage_store.wait()

    @pl.when(c == 1)
    def _():
        def end_sends(e, carry):
            for k, tall in enumerate((8, 16, 8, 8, 16)):
                plane_copy(k, tall, e).wait_send()
            return carry

        lax.fori_loop(1, 16, end_sends, 0)
        for k, tall in enumerate((8, 8, 8, 8, 16, 8, 8, 8)):
            for i in range(7):
                line_copy(k, tall, i).wait_send()

    for d in range(8):
        hand_copy(d).wait_send()
    for d in range(1, 8):
        row_copy(d).wait_send()
        sized(z, lambda width: z_copy(d, width).wait_send())
        sized(source(d), functools.partial(end_parts, d))
    for e in (1, 7, 2):
        back_copy(e).wait_send()


def hand_over(usage_ref, small_ref, usage_out, shared_out, prices_out, primal_out, dual_out):
    usage_out[...] = usage_ref[...]
    shared_out[...] = small_ref[0:1]
    prices_out[...] = small_ref[1:2]
    primal_out[...] = small_ref[2:3, :ITERS]
    dual_out[...] = small_ref[3:4, :ITERS]


def on_device(linear_cost, agent_type, block_mask, inverses, cost_weight, target):
    vmem = pl.BlockSpec(memory_space=pltpu.VMEM)
    anywhere = pl.BlockSpec(memory_space=pl.ANY)
    dma = pltpu.SemaphoreType.DMA
    usage, small = pl.pallas_call(
        kernel,
        out_shape=(jax.ShapeDtypeStruct((256, 256), F32), jax.ShapeDtypeStruct((4, 256), F32)),
        in_specs=[anywhere] * 6,
        out_specs=(anywhere, vmem),
        scratch_shapes=[
            pltpu.VMEM((256, 256), F32),
            pltpu.VMEM((1, 256), jnp.int32),
            pltpu.VMEM((2, 256), jnp.int32),
            pltpu.VMEM((1, 256), F32),
            pltpu.VMEM((1, 256), F32),
            pltpu.VMEM((256, 256), F32),
            pltpu.VMEM((4, 16, 640), BF16),
            pltpu.VMEM((2, 8, 4, 4, 16, 640), BF16),
            pltpu.VMEM((8, 2048, 256), BF16),
            pltpu.VMEM((256, 256), BF16),
            pltpu.VMEM((4, 80, 256), BF16),
            pltpu.VMEM((8, 2, 80, 256), BF16),
            pltpu.VMEM((8, 128, 256), F32),
            pltpu.VMEM((8, 128, 256), F32),
            pltpu.VMEM((144, 2048), BF16),
            pltpu.VMEM((128, 2048), BF16),
            pltpu.VMEM((8, 256), F32),
            pltpu.VMEM((6, 8, 256), F32),
            pltpu.VMEM((ITERS, 16, 16, 256), F32),
            pltpu.VMEM((8, 4, 16, 256), F32),
            pltpu.VMEM((4, 64, 256), F32),
            dma((5,)), dma, dma((20,)), dma((10,)),
            dma((8,)), dma((8,)),
            dma((8, 4)), dma((8, 4)),
            dma((8, 4)), dma((8, 4)),
            dma((8,)), dma((8,)),
            dma((8,)), dma((8,)),
            dma((8,)), dma((8,)),
            dma((ITERS, 16)), dma((ITERS, 16)),
            dma((8, 7)), dma((8, 4)),
            dma((8,)), dma((8,)),
        ],
        compiler_params=pltpu.CompilerParams(
            collective_id=0, has_side_effects=True, vmem_limit_bytes=60 * 2**20
        ),
        name="admm",
    )(
        linear_cost,
        agent_type.reshape(1, -1),
        block_mask.T,
        cost_weight.reshape(1, -1),
        target.reshape(1, -1),
        inverses.reshape(4, 4, 4, 16, 2048),
    )
    usage, shared, prices, primal, dual = pl.pallas_call(
        hand_over,
        out_shape=(
            jax.ShapeDtypeStruct((256, 256), F32),
            jax.ShapeDtypeStruct((1, 256), F32),
            jax.ShapeDtypeStruct((1, 256), F32),
            jax.ShapeDtypeStruct((1, ITERS), F32),
            jax.ShapeDtypeStruct((1, ITERS), F32),
        ),
        in_specs=[vmem] * 2,
        out_specs=(vmem,) * 5,
        name="hand_over",
    )(usage, small)
    return usage, shared.reshape(-1), prices.reshape(-1), primal.reshape(-1), dual.reshape(-1)


def solution(mesh):
    placed = (
        P("agent", "res"),
        P("agent"),
        P("agent", "res"),
        P(None, "res", None),
        P("res"),
        P("res"),
    )
    return jax.shard_map(
        on_device,
        mesh=mesh,
        in_specs=placed,
        out_specs=(P("agent", "res"), P("res"), P("res"), P(), P()),
        check_vma=False,
    )
```

```python
import functools

import jax
import jax.numpy as jnp
from jax import lax
from jax.experimental import pallas as pl
from jax.experimental.pallas import tpu as pltpu
from jax.sharding import PartitionSpec as P

ITERS = 5
LAG_TWO, LAG_THREE, LAG_FOUR = 3, 6, 7
LAST_STEP = LAG_FOUR + 7
AGENTS = 8192
EPS = 1e-06
MESH = pl.DeviceIdType.MESH
F32 = jnp.float32
BF16 = jnp.bfloat16


def three_parts(value):
    high = value.astype(BF16).astype(F32)
    rest = value - high
    mid = rest.astype(BF16).astype(F32)
    return high, mid, rest - mid


def kernel(
    cost_hbm, type_hbm, mask_hbm, weight_hbm, target_hbm, inv_ref,
    usage_hbm, small_out,
    cost_ref, type_ref, mask_ref, weight_ref, target_ref, usage_out, stage, half, full, order, packed, rows, expand, usage, rhs, plain, counts, vectors, plane, lines, back,
    in_load, out_store, stage_load, mat_load, z_send, z_recv, one_send, one_recv, two_send, two_recv, core_send, core_recv,
    row_send, row_recv, hand_send, hand_recv, plane_send, plane_recv, line_send, line_recv, back_send, back_recv,
):
    agent, z = lax.axis_index("agent"), lax.axis_index("res")
    x, y, c = agent // 8, (agent // 2) % 4, agent % 2
    kind = z % 4
    first, second = x * (1 - c) + y * c, y * (1 - c) + x * c
    place = x * 4 + y

    def at(px, py, pc, pz):
        return (px * 8 + py * 2 + pc, pz)

    def along(step_one, step_two):
        one, two = (first + step_one) % 4, (second + step_two) % 4
        return at(one * (1 - c) + two * c, two * (1 - c) + one * c, c, z)

    def copy(src, dst, send, recv, device):
        return pltpu.make_async_remote_copy(src, dst, send, recv, device_id=device, device_id_type=MESH)

    def plane_peer(e):
        other = (place + e) % 16
        return at(other // 4, other % 4, c, z)

    barrier = pltpu.get_barrier_semaphore()

    def greet(e, carry):
        pl.semaphore_signal(barrier, inc=1, device_id=plane_peer(e), device_id_type=MESH)
        return carry

    lax.fori_loop(1, 16, greet, 0)
    for d in range(1, 8):
        pl.semaphore_signal(barrier, inc=1, device_id=at(x, y, c, (z + d) % 8), device_id_type=MESH)
    for d in (0, 1, 7, 2, 6):
        pl.semaphore_signal(barrier, inc=1, device_id=at(x, y, 1 - c, (z + d) % 8), device_id_type=MESH)
    def column(k):
        return pl.ds(pl.multiple_of(((2 * z + k) % 16) * 128, 128), 128)

    in_loads = [
        pltpu.make_async_copy(src, dst, in_load.at[i])
        for i, (src, dst) in enumerate(
            (
                (cost_hbm, cost_ref), (type_hbm, type_ref), (mask_hbm, mask_ref),
                (weight_hbm, weight_ref), (target_hbm, target_ref),
            )
        )
    ]
    for load in in_loads:
        load.start()
    own_loads = [
        pltpu.make_async_copy(
            inv_ref.at[t, first, second, :, column(c * 4 + i + (i // 4) * (4 - 3 * c))],
            stage.at[t, :, pl.ds(i * 128, 128)],
            stage_load.at[t * 5 + i],
        )
        for t in range(4)
        for i in range(5)
    ] + [
        pltpu.make_async_copy(
            inv_ref.at[kind, :, :, :, column(k)],
            half.at[(k // 4 if k < 8 else k - 8), z, :, :, :, pl.ds((k % 4 if k < 8 else 4) * 128, 128)],
            mat_load.at[k],
        )
        for k in range(10)
    ]
    for load in own_loads:
        load.start()
    def sized(source, act):
        @pl.when(source < 4)
        def _():
            act(640)

        @pl.when(source >= 4)
        def _():
            act(512)

    def z_copy(d, width):
        far = (z + d) % 8
        return copy(
            stage.at[far % 4, :, :width],
            half.at[c, z, first, second, :, :width],
            z_send.at[d],
            z_recv.at[d],
            at(x, y, c, far),
        )

    for load in own_loads[:20]:
        load.wait()
    pl.semaphore_wait(barrier, 27)

    def start_parts(width):
        for d in (1, 7, 2, 6, 3, 5, 4):
            z_copy(d, width).start()

    sized(z, start_parts)

    for load in in_loads:
        load.wait()
    kinds = type_ref[...]
    is_kind = (lax.broadcasted_iota(jnp.int32, (16, 256), 0) == kinds).astype(F32)
    before = (
        lax.broadcasted_iota(jnp.int32, (256, 256), 0) < lax.broadcasted_iota(jnp.int32, (256, 256), 1)
    ).astype(BF16)
    ahead = jnp.dot(is_kind.astype(BF16), before, preferred_element_type=F32)
    spot = kinds * 64 + jnp.sum(is_kind * ahead, axis=0, keepdims=True).astype(jnp.int32)
    order[...] = (lax.broadcasted_iota(jnp.int32, (256, 256), 0) == spot).astype(F32).astype(BF16)
    cost = jnp.dot(order[...], cost_ref[...].astype(BF16), preferred_element_type=F32).astype(BF16)
    extra = jnp.concatenate(
        [mask_ref[...].astype(F32), jnp.zeros((14, 256), F32)], axis=0
    ).astype(BF16)
    masks = lax.dot_general(extra, order[...], (((1,), (1,)), ((), ())), preferred_element_type=F32)
    line = lax.broadcasted_iota(jnp.int32, (16, 256), 0)
    lane = lax.broadcasted_iota(jnp.int32, (16, 256), 1)
    tail = jnp.zeros((16, 256), F32)
    for r, part in enumerate(three_parts(weight_ref[...]) + three_parts(target_ref[...])):
        tail = jnp.where(line == 2 + r, part, tail)
    for t in range(4):
        packed[t, :64] = cost[t * 64 : (t + 1) * 64]
        turned = masks if t == 0 else pltpu.roll(masks, 256 - 64 * t, 1)
        packed[t, 64:] = jnp.where((line < 2) & (lane < 64), turned, tail)[:8].astype(BF16)

    def row_copy(d):
        far = (z + d) % 8
        return copy(packed.at[far % 4], rows.at[z, c], row_send.at[d], row_recv.at[d], at(x, y, c, far))

    def hand_copy(d):
        block = rows.at[(z - d + 8) % 8, c]
        return copy(block, block, hand_send.at[d], hand_recv.at[d], at(x, y, 1 - c, z))

    for d in (1, 7, 2, 6, 3, 5, 4):
        row_copy(d).start()
    rows[z, c] = packed[kind]
    hand_copy(0).start()

    def source(d):
        return (z - d + 8) % 8

    def one_copy(d, s, width):
        block = half.at[c, source(d), first, second, :, :width]
        return copy(block, block, one_send.at[d, s], one_recv.at[d, s], along(s, 0))

    def two_copy(d, s, width):
        block = half.at[c, source(d), :, second, :, :width]
        return copy(block, block, two_send.at[d, s], two_recv.at[d, s], along(0, s))

    def core_copy(d, width):
        block = half.at[c, source(d), :, :, :, :width]
        return copy(block, block, core_send.at[d], core_recv.at[d], at(x, y, 1 - c, z))

    line = lax.broadcasted_iota(jnp.int32, (16, 256), 0)
    wide = (lax.broadcasted_iota(jnp.int32, (16, 256), 1) // 128 == line).astype(F32).astype(BF16)

    def fill_tiles(block, picked):
        for k in picked:
            side, spot_ = (k // 4, k % 4) if k < 8 else (k - 8, 4)
            tile = half[side, block, :, :, :, spot_ * 128 : spot_ * 128 + 128].reshape(256, 128)
            across = (block + k // 2) % 8
            full[across, pl.ds(pl.multiple_of(block * 256, 256), 256), (k % 2) * 128 : (k % 2) * 128 + 128] = tile
            if k >= 2:
                full[block, pl.ds(pl.multiple_of(across * 256 + (k % 2) * 128, 128), 128), :] = tile.T

    def times(row_block, column_block):
        return jnp.dot(
            rows[row_block, :, :64].reshape(128, 256),
            full[column_block, pl.ds(pl.multiple_of(row_block * 256, 256), 256), :],
            preferred_element_type=F32,
        )

    def fill(block):
        fill_tiles(block, range(8))
        for j in range(4):
            across = (block + j) % 8
            usage[across] += times(block, across)
        mirror = jnp.zeros((128, 256), F32)
        for j in range(1, 4):
            mirror += times((block + j) % 8, block)
        usage[block] += mirror

        @pl.when(block < 4)
        def _():
            across = (block + 4) % 8
            fill_tiles(block, (8, 9))
            usage[across] += times(block, across)
            usage[block] += times(across, block)

    def stage_one(d, width):
        z_copy(d, width).wait_recv()
        for s in (2, 1, 3):
            one_copy(d, s, width).start()

    def stage_two(d, width):
        for s in (2, 1, 3):
            one_copy(d, s, width).wait_recv()
        for s in (2, 1, 3):
            two_copy(d, s, width).start()

    def stage_three(d, width):
        for s in (2, 1, 3):
            two_copy(d, s, width).wait_recv()
        core_copy(d, width).start()

    def stage_four(d, width):
        core_copy(d, width).wait_recv()

    def end_parts(d, width):
        for s in (1, 2, 3):
            one_copy(d, s, width).wait_send()
            two_copy(d, s, width).wait_send()
        core_copy(d, width).wait_send()

    def unpack():
        for d in (1, 7, 2, 6, 3, 5, 4):
            row_copy(d).wait_recv()
            hand_copy(d).start()
        for load in own_loads[20:]:
            load.wait()
        for d in range(8):
            hand_copy(d).wait_recv()
        for j in range(8):
            ends = rows[j, 0, 64:].astype(F32)
            vectors[0, j : j + 1] = ends[2:3] + ends[3:4] + ends[4:5]
            vectors[1, j : j + 1] = ends[5:6] + ends[6:7] + ends[7:8]
            for side in range(2):
                here = rows[j, side, 64:, :128]
                spread = lax.dot_general(here, wide[:8], (((0,), (0,)), ((), ())), preferred_element_type=F32)
                expand[j, side * 64 : side * 64 + 64] = spread[:64]
        usage[...] = jnp.zeros((8, 128, 256), F32)
        fill(z)

    turns = (1, 7, 2, 6, 3, 5, 4)
    for step in range(LAST_STEP):
        for lag, act in ((0, stage_one), (LAG_TWO, stage_two), (LAG_THREE, stage_three), (LAG_FOUR, stage_four)):
            if 0 <= step - lag < 7:
                sized(source(turns[step - lag]), functools.partial(act, turns[step - lag]))
                if act is stage_four:
                    fill(source(turns[step - lag]))
        if step == LAG_FOUR - 1:
            unpack()

    norm_lane = lax.broadcasted_iota(jnp.int32, (1, 128), 1)

    def back_copy(e):
        far = (z + e) % 8
        return copy(
            usage.at[far, pl.ds(pl.multiple_of(c * 64, 64), 64)],
            back.at[kind],
            back_send.at[e],
            back_recv.at[e],
            at(x, y, c, far),
        )

    def place_columns(k, j, value):
        plane[k, place, pl.ds(j, 1)] = jnp.sum(value, axis=0, keepdims=True)

    def plane_copy(k, tall, e):
        block = plane.at[k, place, pl.ds(0, tall)]
        return copy(block, block, plane_send.at[k, e], plane_recv.at[k, e], plane_peer(e))

    def start_plane(k, tall):
        @pl.when(c == 1)
        def _():
            def start(e, carry):
                plane_copy(k, tall, e).start()
                return carry

            lax.fori_loop(1, 16, start, 0)

    def line_copy(k, tall, i):
        e = i // 2
        far = at(x, y, 1 - c, z) if e == 3 else at(x, y, 1 - i % 2, (z + (1, 7, 2)[e]) % 8)
        block = lines.at[k, kind, pl.ds(0, tall)]
        return copy(block, block, line_send.at[k, i], line_recv.at[k, e], far)

    def start_line(k, value):
        tall = value.shape[0]
        lines[k, kind, :tall] = value
        for i in range(7):
            line_copy(k, tall, i).start()

    def relay(k, tall):
        @pl.when(c == 1)
        def _():
            def end(e, carry):
                plane_copy(k, tall, e).wait_recv()
                return carry

            lax.fori_loop(1, 16, end, 0)
            sums = jnp.sum(plane[k, :, :tall], axis=0)
            if k == 1:
                start_line(k, sums[:8])
                counts[...] = sums[8:]
            else:
                start_line(k, sums)

    def end_line(k, tall):
        for e in range(3):
            line_copy(k, tall, 2 * e).wait_recv()

        @pl.when(c == 0)
        def _():
            line_copy(k, tall, 6).wait_recv()

        return jnp.sum(lines[k, :, :tall], axis=0)

    def block_of(j):
        return full[j]

    def lanes_of(j):
        return pl.ds(pl.multiple_of(j * 256, 256), 256)

    def costs_of(j):
        return rows[j, :, :64].astype(F32).reshape(128, 256)

    def opened(j):
        return jnp.dot(plain[...], block_of(j), preferred_element_type=F32)

    def applied(k):
        def step(j, carry):
            place_columns(k, j, opened(j) * expand[j])
            return carry

        lax.fori_loop(0, 8, step, 0, unroll=8)

    def advance(k, v, ex=None):
        vectors[4] = v
        high, mid, low = three_parts(v)
        for j in range(8):
            rhs[:128, j * 256 : (j + 1) * 256] = (usage[j] + vectors[4, j : j + 1] - costs_of(j)).astype(BF16)
            stack = jnp.where(line == 0, high[j : j + 1], jnp.where(line == 1, mid[j : j + 1], low[j : j + 1]))
            rhs[128:, j * 256 : (j + 1) * 256] = jnp.where(line < 3, stack, 0.0).astype(BF16)

        def step(j, change):
            both = jnp.dot(rhs[...], block_of(j), preferred_element_type=F32)
            vectors[4, pl.ds(j, 1)] = both[128:129] + both[129:130] + both[130:131]
            fresh = both[:128] * expand[j]
            gap = fresh - usage[j]
            usage[j] = fresh
            if ex is not None:
                plain[:, lanes_of(j)] = (fresh - costs_of(j)).astype(BF16)
            return change + jnp.sum(gap * gap, axis=0, keepdims=True)

        change = lax.fori_loop(0, 8, step, jnp.zeros((1, 256), F32), unroll=8)
        if ex is not None:
            plane[4, place, 7 + k : 8 + k] = change

            @pl.when(c == 1)
            def _():
                start_line(ex, counts[...] * vectors[4])

    def foreseen():
        vectors[5] = vectors[4]

        def step(j, change):
            gap = (opened(j) + vectors[5, pl.ds(j, 1)]) * expand[j] - usage[j]
            place_columns(4, j, gap)
            return change + jnp.sum(gap * gap, axis=0, keepdims=True)

        plane[4, place, 12:13] = lax.fori_loop(0, 8, step, jnp.zeros((1, 256), F32), unroll=8)
        plane[4, place, 13:] = jnp.zeros((3, 256), F32)

    def relay_last():
        @pl.when(c == 1)
        def _():
            def end(e, carry):
                plane_copy(4, 16, e).wait_recv()
                return carry

            lax.fori_loop(1, 16, end, 0)
            sums = jnp.sum(plane[4], axis=0)
            step = vectors[4] - vectors[5]
            gaps, masks_ = sums[:8], counts[...]
            square = jnp.sum((2.0 * gaps + masks_ * step) * step, axis=0, keepdims=True)
            row = lax.broadcasted_iota(jnp.int32, (8, 256), 0)
            tail_ = sums[8:] + jnp.where(row == 4, square, 0.0)
            start_line(4, jnp.concatenate([gaps + masks_ * step, tail_], axis=0))

    def settle(total, prices, norms, k):
        mean = total * (1.0 / AGENTS)
        shared = (vectors[0] * vectors[1] + (prices + mean)) / (vectors[0] + 1.0)
        prices = prices + mean - shared
        gap = mean - shared
        norms = jnp.where(norm_lane == k - 1, float(AGENTS) * jnp.sum(gap * gap), norms)
        return shared - mean - prices, shared, prices, norms

    def opening(j, change):
        fresh = -usage[j] * expand[j]
        usage[j] = fresh
        plain[:, lanes_of(j)] = (fresh - costs_of(j)).astype(BF16)
        place_columns(0, j, fresh)
        return change + jnp.sum(fresh * fresh, axis=0, keepdims=True)

    plane[4, place, 8:9] = lax.fori_loop(0, 8, opening, jnp.zeros((1, 256), F32), unroll=8)
    start_plane(0, 8)
    for j in range(8):
        plane[1, place, 8 + j : 9 + j] = jnp.sum(expand[j], axis=0, keepdims=True)
    applied(1)
    start_plane(1, 16)
    relay(0, 8)
    relay(1, 16)
    norms = jnp.zeros((1, 128), F32)
    v, shared, prices, norms = settle(end_line(0, 8), jnp.zeros((8, 256), F32), norms, 1)
    advance(2, v, ex=5)
    applied(2)
    start_plane(2, 8)
    v, shared, prices, norms = settle(end_line(1, 8) + end_line(5, 8), prices, norms, 2)
    advance(3, v, ex=6)
    applied(3)
    start_plane(3, 8)
    relay(2, 8)
    v, shared, prices, norms = settle(end_line(2, 8) + end_line(6, 8), prices, norms, 3)
    advance(4, v, ex=7)
    relay(3, 8)
    foreseen()
    start_plane(4, 16)
    usage_sum = end_line(3, 8) + end_line(7, 8)
    v, shared, prices, norms = settle(usage_sum, prices, norms, 4)
    advance(5, v)
    for e in (1, 7, 2):
        back_copy(e).start()
    back[kind] = usage[z, pl.ds(pl.multiple_of(c * 64, 64), 64)]
    relay_last()
    for e in (1, 7, 2):
        back_copy(e).wait_recv()
    result = jnp.zeros((256, 256), F32)
    for piece in three_parts(back[...].reshape(256, 256)):
        result += lax.dot_general(
            order[...], piece.astype(BF16), (((0,), (0,)), ((), ())), preferred_element_type=F32
        )
    usage_out[...] = result
    usage_store = pltpu.make_async_copy(usage_out, usage_hbm, out_store)
    usage_store.start()
    total = end_line(4, 16)
    v, shared, prices, norms = settle(usage_sum + total[:8], prices, norms, 5)
    duals = jnp.zeros((1, 128), F32)
    for k in range(ITERS):
        duals = jnp.where(norm_lane == k, jnp.sum(total[8 + k : 9 + k]), duals)
    vectors[2] = shared
    vectors[3] = prices
    small_out[0:1] = vectors[2, pl.ds(z, 1)]
    small_out[1:2] = vectors[3, pl.ds(z, 1)]
    small_out[2:3, :128] = jnp.sqrt(norms + EPS)
    small_out[3:4, :128] = jnp.sqrt(duals + EPS)
    usage_store.wait()

    @pl.when(c == 1)
    def _():
        def end_sends(e, carry):
            for k, tall in enumerate((8, 16, 8, 8, 16)):
                plane_copy(k, tall, e).wait_send()
            return carry

        lax.fori_loop(1, 16, end_sends, 0)
        for k, tall in enumerate((8, 8, 8, 8, 16, 8, 8, 8)):
            for i in range(7):
                line_copy(k, tall, i).wait_send()

    for d in range(8):
        hand_copy(d).wait_send()
    for d in range(1, 8):
        row_copy(d).wait_send()
        sized(z, lambda width: z_copy(d, width).wait_send())
        sized(source(d), functools.partial(end_parts, d))
    for e in (1, 7, 2):
        back_copy(e).wait_send()


def hand_over(usage_ref, small_ref, usage_out, shared_out, prices_out, primal_out, dual_out):
    usage_out[...] = usage_ref[...]
    shared_out[...] = small_ref[0:1]
    prices_out[...] = small_ref[1:2]
    primal_out[...] = small_ref[2:3, :ITERS]
    dual_out[...] = small_ref[3:4, :ITERS]


def on_device(linear_cost, agent_type, block_mask, inverses, cost_weight, target):
    vmem = pl.BlockSpec(memory_space=pltpu.VMEM)
    anywhere = pl.BlockSpec(memory_space=pl.ANY)
    dma = pltpu.SemaphoreType.DMA
    usage, small = pl.pallas_call(
        kernel,
        out_shape=(jax.ShapeDtypeStruct((256, 256), F32), jax.ShapeDtypeStruct((4, 256), F32)),
        in_specs=[anywhere] * 6,
        out_specs=(anywhere, vmem),
        scratch_shapes=[
            pltpu.VMEM((256, 256), F32),
            pltpu.VMEM((1, 256), jnp.int32),
            pltpu.VMEM((2, 256), jnp.int32),
            pltpu.VMEM((1, 256), F32),
            pltpu.VMEM((1, 256), F32),
            pltpu.VMEM((256, 256), F32),
            pltpu.VMEM((4, 16, 640), BF16),
            pltpu.VMEM((2, 8, 4, 4, 16, 640), BF16),
            pltpu.VMEM((8, 2048, 256), BF16),
            pltpu.VMEM((256, 256), BF16),
            pltpu.VMEM((4, 72, 256), BF16),
            pltpu.VMEM((8, 2, 72, 256), BF16),
            pltpu.VMEM((8, 128, 256), F32),
            pltpu.VMEM((8, 128, 256), F32),
            pltpu.VMEM((144, 2048), BF16),
            pltpu.VMEM((128, 2048), BF16),
            pltpu.VMEM((8, 256), F32),
            pltpu.VMEM((6, 8, 256), F32),
            pltpu.VMEM((ITERS, 16, 16, 256), F32),
            pltpu.VMEM((8, 4, 16, 256), F32),
            pltpu.VMEM((4, 64, 256), F32),
            dma((5,)), dma, dma((20,)), dma((10,)),
            dma((8,)), dma((8,)),
            dma((8, 4)), dma((8, 4)),
            dma((8, 4)), dma((8, 4)),
            dma((8,)), dma((8,)),
            dma((8,)), dma((8,)),
            dma((8,)), dma((8,)),
            dma((ITERS, 16)), dma((ITERS, 16)),
            dma((8, 7)), dma((8, 4)),
            dma((8,)), dma((8,)),
        ],
        compiler_params=pltpu.CompilerParams(
            collective_id=0, has_side_effects=True, vmem_limit_bytes=60 * 2**20
        ),
        name="admm",
    )(
        linear_cost,
        agent_type.reshape(1, -1),
        block_mask.T,
        cost_weight.reshape(1, -1),
        target.reshape(1, -1),
        inverses.reshape(4, 4, 4, 16, 2048),
    )
    usage, shared, prices, primal, dual = pl.pallas_call(
        hand_over,
        out_shape=(
            jax.ShapeDtypeStruct((256, 256), F32),
            jax.ShapeDtypeStruct((1, 256), F32),
            jax.ShapeDtypeStruct((1, 256), F32),
            jax.ShapeDtypeStruct((1, ITERS), F32),
            jax.ShapeDtypeStruct((1, ITERS), F32),
        ),
        in_specs=[vmem] * 2,
        out_specs=(vmem,) * 5,
        name="hand_over",
    )(usage, small)
    return usage, shared.reshape(-1), prices.reshape(-1), primal.reshape(-1), dual.reshape(-1)


def solution(mesh):
    placed = (
        P("agent", "res"),
        P("agent"),
        P("agent", "res"),
        P(None, "res", None),
        P("res"),
        P("res"),
    )
    return jax.shard_map(
        on_device,
        mesh=mesh,
        in_specs=placed,
        out_specs=(P("agent", "res"), P("res"), P("res"), P(), P()),
        check_vma=False,
    )
```
